32 devices in a mesh: inp: 4 (over x, core), out: 8 (over z, y).
Axes of the slice: x: 2, y: 2, z: 4, core: 2. Of those that a mesh axis runs over, the one named last changes fastest.
Arguments:
- attention: bfloat16 [128, 16384], P(None, ('inp', 'out')), may hold values from -6 to 6
- residual: bfloat16 [128, 16384], P(None, 'out'), may hold values from -60 to 60
- wo_codes: int32 [2, 2048, 16384], P(None, 'inp', 'out'), may hold values from 0 to 255
- wo_books: bfloat16 [2, 256, 8], replicated, may hold values from -0.03125 to 0.03125
- wo_scale: float32 [16384], P('out'), may hold values from 0.5 to 2
- norm_gain: float32 [16384], replicated, may hold values from 0.25 to 1.75
- gate_codes: int32 [2, 2048, 53248], P(None, 'inp', 'out'), may hold values from 0 to 255
- gate_books: bfloat16 [2, 256, 8], replicated, may hold values from -0.03125 to 0.03125
- gate_scale: float32 [53248], P('out'), may hold values from 0.5 to 2
Outputs:
- stream: bfloat16 [128, 16384], P(None, 'out')
- gate_out: bfloat16 [128, 53248], P('inp', 'out')
The draws below stay inside these ranges and needn't reach their ends.
All inputs are finite; a program needn't handle non-finite values.
Results may differ from the reference program's by a relative error of at most 0.0059.
Values may be sent and summed in bfloat16 or wider, within the bound.
No kernel may reach another device: no remote copies, remote signals or barrier semaphores. Data moves between devices by JAX's collectives and lax.ppermute only.
A program may use at most 192 MiB of HBM per device.

```python
import math
import jax
import jax.numpy as jnp
from jax import lax

D = 16384
FF = 53248
B = 128
BOOK = 256
GROUP = 8


def draw_residual(key, part):
    key_row, key_col, key_val = jax.random.split(key, 3)
    position = jnp.linspace(0.0, 1.0, D, dtype=jnp.float32)[None, :]
    rough = jax.random.uniform(key_col, (1, D), jnp.float32, 0.5, 1.5)
    row_scale = jnp.exp(jax.random.uniform(key_row, (B, 1), jnp.float32, jnp.log(0.3), jnp.log(3.0)))
    ramp = jnp.exp(position * jnp.log(3.0))
    values = jnp.clip(jax.random.normal(key_val, (B, D), jnp.float32), -6.0, 6.0)
    result = jnp.clip(values * row_scale * ramp * rough, -60.0, 60.0)
    return result.astype(jnp.bfloat16)


def with_ends(drawn, rng, low, top_value):
    extent = drawn.shape
    index_at = [jax.random.randint(jax.random.fold_in(rng, axis), (), 0, extent[axis]) for axis in range(len(extent))]
    drawn = drawn.at[tuple(index_at)].set(low)
    longest = extent.index(max(extent))
    index_at[longest] = (index_at[longest] + 1) % extent[longest]
    return drawn.at[tuple(index_at)].set(top_value)


def shard_levels(rng, extent, cuts, low, top_value):
    loudness = 1.0
    for axis_at, shards_of in cuts:
        draws = jax.random.uniform(jax.random.fold_in(jax.random.fold_in(rng, 6), axis_at), (shards_of,), jnp.float32, low / len(cuts), top_value / len(cuts))
        loudness = loudness * jnp.repeat(jnp.exp(draws), extent[axis_at] // shards_of).reshape((-1,) + (1,) * (len(extent) - 1 - axis_at))
    return loudness


def scatter_about(stream_key, shape, scale, limit, pieces=(), kind=jnp.bfloat16):
    loudness = shard_levels(stream_key, shape, pieces, -0.22, 0.18) if pieces else 1.0
    entries = jax.random.normal(stream_key, shape, jnp.float32) * scale * loudness
    return jnp.minimum(jnp.maximum(entries, -limit), limit).astype(kind)


def setup_inputs(seed: int = 0) -> dict:
    streams_of = jax.random.split(jax.random.key(seed), 10)
    attention = scatter_about(streams_of[0], (B, D), 1.0, 6.0, ((1, 32),))
    residual = draw_residual(jax.random.fold_in(streams_of[9], 71), 0)
    wo_codes = with_ends(jax.random.randint(streams_of[2], (2, D // GROUP, D), 0, BOOK), jax.random.fold_in(streams_of[2], 1), 0, BOOK - 1).astype(jnp.int32)
    wo_books = scatter_about(streams_of[3], (2, BOOK, GROUP), (2 * D) ** -0.5, 0.03125)
    wo_scale = jnp.clip(jnp.exp(math.log(2.0) - 1.3862944 * jax.random.uniform(streams_of[4], (D,), jnp.float32) ** shard_levels(streams_of[4], (D,), ((0, 8),), -0.2, 0.2)), 0.5, 2.0)
    norm_gain = jnp.clip(1.0 + 0.15 * jax.random.normal(streams_of[5], (D,), jnp.float32), 0.25, 1.75)
    gate_codes = with_ends(jax.random.randint(streams_of[6], (2, D // GROUP, FF), 0, BOOK), jax.random.fold_in(streams_of[6], 1), 0, BOOK - 1).astype(jnp.int32)
    gate_books = scatter_about(streams_of[7], (2, BOOK, GROUP), (2 * D) ** -0.5, 0.03125)
    gate_scale = jnp.clip(jnp.exp(math.log(2.0) - 1.3862944 * jax.random.uniform(streams_of[8], (FF,), jnp.float32) ** shard_levels(streams_of[8], (FF,), ((0, 8),), -0.2, 0.2)), 0.5, 2.0)
    return dict(attention=attention, residual=residual, wo_codes=wo_codes, wo_books=wo_books, wo_scale=wo_scale, norm_gain=norm_gain, gate_codes=gate_codes, gate_books=gate_books, gate_scale=gate_scale)


epsilon = 1e-05

def decompress(codes, books, scale):
    tables = books.astype(jnp.float32)
    first_book = jnp.take(tables[0], codes[0], axis=0)
    second_book = jnp.take(tables[1], codes[1], axis=0)
    summed = first_book + second_book
    groups, outputs = (codes.shape[1], codes.shape[2])
    weight = jnp.transpose(summed, (0, 2, 1)).reshape(groups * GROUP, outputs) * scale[None, :]
    return weight.astype(jnp.bfloat16)

def project(inputs, codes, books, scale):
    groups, outputs = (codes.shape[1], codes.shape[2])
    block_width = math.gcd(outputs, 1024)
    block_count = outputs // block_width
    code_blocks = jnp.transpose(codes.reshape(2, groups, block_count, block_width), (2, 0, 1, 3))
    scale_blocks = scale.reshape(block_count, block_width)

    def one_block(pair):
        weight = decompress(pair[0], books, pair[1])
        return jnp.dot(inputs, weight, preferred_element_type=jnp.float32)
    result = lax.map(one_block, (code_blocks, scale_blocks))
    return jnp.transpose(result, (1, 0, 2)).reshape(inputs.shape[0], outputs)

def reference(attention, residual, wo_codes, wo_books, wo_scale, norm_gain, gate_codes, gate_books, gate_scale):
    projected = project(attention, wo_codes, wo_books, wo_scale)
    hidden = residual.astype(jnp.float32) + projected
    square_mean = lax.optimization_barrier(jnp.mean(hidden * hidden, axis=1, keepdims=True))
    normed = (hidden * lax.rsqrt(square_mean + epsilon) * norm_gain[None, :]).astype(jnp.bfloat16)
    gate_out = project(normed, gate_codes, gate_books, gate_scale).astype(jnp.bfloat16)
    return (hidden.astype(jnp.bfloat16), gate_out)
```

```python
import functools
import math

import jax
import jax.numpy as jnp
from jax import lax
from jax.experimental import pallas as pl
from jax.experimental.pallas import tpu as pltpu
from jax.sharding import PartitionSpec as P

epsilon = 1e-05
LANES = 128
SUBLANES = 8
LEVELS = 16383.0
HALF = 65536.0

take_lanes = lax.GatherDimensionNumbers(
    offset_dims=(),
    collapsed_slice_dims=(1,),
    start_index_map=(1,),
    operand_batching_dims=(0,),
    start_indices_batching_dims=(0,),
)


def lookup(table, index):
    return lax.gather(
        table,
        index[..., None],
        take_lanes,
        slice_sizes=(1, 1),
        mode=lax.GatherScatterMode.PROMISE_IN_BOUNDS,
    )


def pack_books(books):
    values = books.astype(jnp.float32)
    top = jnp.maximum(jnp.max(jnp.abs(values)), 1e-30)
    levels = jnp.round(values * (LEVELS / top)).astype(jnp.int32)
    books_count, entries, group = levels.shape
    words = levels[:, :, 0::2] * 65536 + levels[:, :, 1::2]
    halves = entries // LANES
    words = words.reshape(books_count, halves, LANES, group // 2)
    words = jnp.transpose(words, (0, 1, 3, 2)).reshape(-1, LANES)
    return words, top / (LEVELS * HALF)


def decode_block(codes, tables):
    words = tables[0][0]
    picked = []
    for book, code in enumerate(codes):
        low = code < LANES
        index = code & (LANES - 1)
        first = [lookup(t, index) for t in tables[book][0]]
        second = [lookup(t, index) for t in tables[book][1]]
        picked.append([jnp.where(low, a, b) for a, b in zip(first, second)])
    rows = []
    for w in range(len(words)):
        both = picked[0][w] + picked[1][w]
        rows.append(both.astype(jnp.float32))
        rows.append((both << 16).astype(jnp.float32))
    return jnp.concatenate(rows, axis=0).astype(jnp.bfloat16)


def project_kernel(chunk, x_ref, codes_ref, table_ref, scale_ref, out_ref, x_perm, w_even, w_odd, total):
    features = x_ref.shape[1]
    width = out_ref.shape[1]
    words = table_ref.shape[0] // 4
    chunks = features // chunk
    blocks = chunk // 64

    @pl.when(pl.program_id(0) == 0)
    def _():
        row = lax.broadcasted_iota(jnp.int32, (LANES, LANES), 0)
        col = lax.broadcasted_iota(jnp.int32, (LANES, LANES), 1)
        source = (col // 64) * 64 + (col % 8) * 8 + (col % 64) // 8
        swap = jnp.where(row == source, 1.0, 0.0).astype(jnp.bfloat16)
        for c in range(features // LANES):
            at = slice(c * LANES, (c + 1) * LANES)
            x_perm[:, at] = jnp.dot(
                x_ref[:, at], swap, preferred_element_type=jnp.float32
            ).astype(jnp.bfloat16)

    def decode(c, w_ref):
        tables = [
            [
                [
                    jnp.broadcast_to(
                        table_ref[(book * 2 + half) * words + w : (book * 2 + half) * words + w + 1, :],
                        (SUBLANES, LANES),
                    )
                    for w in range(words)
                ]
                for half in range(2)
            ]
            for book in range(2)
        ]
        for b in range(blocks):
            first = pl.multiple_of(c * (chunk // 8) + b * SUBLANES, SUBLANES)
            for j in range(0, width, LANES):
                codes = [codes_ref[book, pl.ds(first, SUBLANES), j : j + LANES] for book in range(2)]
                w_ref[b * 64 : (b + 1) * 64, j : j + LANES] = decode_block(codes, tables)

    def multiply(c, w_ref):
        at = pl.ds(pl.multiple_of(c * chunk, chunk), chunk)
        total[...] += jnp.dot(x_perm[:, at], w_ref[...], preferred_element_type=jnp.float32)

    total[...] = jnp.zeros_like(total)
    w_odd[...] = jnp.zeros_like(w_odd)

    def pair(i, carry):
        decode(2 * i, w_even)
        multiply(jnp.maximum(2 * i - 1, 0), w_odd)
        decode(2 * i + 1, w_odd)
        multiply(2 * i, w_even)
        return carry

    lax.fori_loop(0, chunks // 2, pair, 0)
    multiply(chunks - 1, w_odd)
    out_ref[...] = (total[...] * scale_ref[...]).astype(out_ref.dtype)


def project(x, codes, table, scale, name, out_dtype=jnp.float32):
    rows, features = x.shape
    _, groups, outputs = codes.shape
    width = math.gcd(outputs, 512)
    chunk = min(512, features // 2)
    steps = outputs // width
    return pl.pallas_call(
        functools.partial(project_kernel, chunk),
        grid=(steps,),
        in_specs=[
            pl.BlockSpec((rows, features), lambda n: (0, 0)),
            pl.BlockSpec((2, groups, width), lambda n: (0, 0, n)),
            pl.BlockSpec(table.shape, lambda n: (0, 0)),
            pl.BlockSpec((1, width), lambda n: (0, n)),
        ],
        out_specs=pl.BlockSpec((rows, width), lambda n: (0, n)),
        out_shape=jax.ShapeDtypeStruct((rows, outputs), out_dtype),
        scratch_shapes=[
            pltpu.VMEM((rows, features), jnp.bfloat16),
            pltpu.VMEM((chunk, width), jnp.bfloat16),
            pltpu.VMEM((chunk, width), jnp.bfloat16),
            pltpu.VMEM((rows, width), jnp.float32),
        ],
        compiler_params=pltpu.CompilerParams(vmem_limit_bytes=24 * 1024 * 1024),
        cost_estimate=pl.CostEstimate(
            flops=2 * rows * features * outputs,
            bytes_accessed=8 * groups * outputs + 4 * rows * outputs + 2 * rows * features,
            transcendentals=0,
        ),
        name=name,
    )(x, codes, table, scale)


def per_device(
    attention, residual, wo_codes, wo_books, wo_scale, norm_gain, gate_codes, gate_books, gate_scale
):
    inp = lax.axis_size("inp")
    out = lax.axis_size("out")
    inp_at = lax.axis_index("inp")
    out_at = lax.axis_index("out")
    model = norm_gain.shape[0]
    features = lax.all_gather(attention, "out", axis=1, tiled=True)
    wo_table, wo_factor = pack_books(wo_books)
    gate_table, gate_factor = pack_books(gate_books)

    partial = project(features, wo_codes, wo_table, (wo_scale * wo_factor)[None, :], "wo_project")
    summed = lax.psum_scatter(partial, "inp", scatter_dimension=1, tiled=True)
    piece = summed.shape[1]
    kept = lax.dynamic_slice_in_dim(residual, inp_at * piece, piece, 1)
    hidden = kept.astype(jnp.float32) + summed
    stream = lax.all_gather(hidden.astype(jnp.bfloat16), "inp", axis=1, tiled=True)
    gain = lax.dynamic_slice_in_dim(norm_gain, (out_at * inp + inp_at) * piece, piece, 0)
    gained = (hidden * gain[None, :]).astype(jnp.bfloat16)
    squares = lax.psum(jnp.sum(hidden * hidden, axis=1, keepdims=True), ("inp", "out"))

    per_block = out // inp
    moves = [
        (q * out + o, (o // per_block) * out + (o % per_block) * inp + q)
        for q in range(inp)
        for o in range(out)
    ]
    moved = lax.ppermute(gained, ("inp", "out"), moves)
    gate_in = lax.all_gather(moved, "out", axis=1, tiled=True)
    gate_partial = project(
        gate_in, gate_codes, gate_table, (gate_scale * gate_factor)[None, :], "gate_project"
    )
    gate_sum = lax.psum_scatter(gate_partial, "inp", scatter_dimension=0, tiled=True)
    own_rows = gate_sum.shape[0]
    row_factor = lax.rsqrt(
        lax.dynamic_slice_in_dim(squares, inp_at * own_rows, own_rows, 0) / model + epsilon
    )
    gate_out = (gate_sum * row_factor).astype(jnp.bfloat16)
    return (stream, gate_out)


def solution(mesh):
    placed = (
        P(None, ("inp", "out")),
        P(None, "out"),
        P(None, "inp", "out"),
        P(),
        P("out"),
        P(),
        P(None, "inp", "out"),
        P(),
        P("out"),
    )
    return jax.shard_map(
        per_device,
        mesh=mesh,
        in_specs=placed,
        out_specs=(P(None, "out"), P("inp", "out")),
        check_vma=False,
    )
```

```python
import functools
import math

import jax
import jax.numpy as jnp
from jax import lax
from jax.experimental import pallas as pl
from jax.experimental.pallas import tpu as pltpu
from jax.sharding import PartitionSpec as P


epsilon = 1e-05
LANES = 128
GROUP = 8
ROWS = 16
BLOCK = ROWS * GROUP
MIB = 1024 * 1024

take_lanes = lax.GatherDimensionNumbers(
    offset_dims=(),
    collapsed_slice_dims=(1,),
    start_index_map=(1,),
    operand_batching_dims=(0,),
    start_indices_batching_dims=(0,),
)


def lookup(table, index):
    return lax.gather(
        table,
        index[..., None],
        take_lanes,
        slice_sizes=(1, 1),
        mode=lax.GatherScatterMode.PROMISE_IN_BOUNDS,
    )


def spread_books(books):
    count, entries, group = books.shape
    halves = entries // LANES
    rows = jnp.transpose(books.reshape(count, halves, LANES, group), (0, 1, 3, 2))
    rows = rows.reshape(count * halves * group, 1, LANES)
    return jnp.broadcast_to(rows, (count * halves * group, ROWS, LANES))


def decode_block(codes, table_ref):
    lows, indices = [], []
    for code in codes:
        narrow = code.astype(jnp.int16)
        lows.append(narrow < LANES)
        indices.append(narrow & (LANES - 1))
    picked = []
    for book in range(2):
        first = [lookup(table_ref[(book * 2) * GROUP + k], indices[book]) for k in range(GROUP)]
        second = [lookup(table_ref[(book * 2 + 1) * GROUP + k], indices[book]) for k in range(GROUP)]
        picked.append([jnp.where(lows[book], a, b) for a, b in zip(first, second)])
    return [a + b for a, b in zip(*picked)]


def decode_rows(first_block, blocks, width, codes_ref, table_ref, w_ref, first_row):
    for b in range(blocks):
        groups = pl.ds(pl.multiple_of((first_block + b) * ROWS, ROWS), ROWS)
        for j in range(0, width, LANES):
            codes = [codes_ref[book, groups, j : j + LANES] for book in range(2)]
            for k, rows in enumerate(decode_block(codes, table_ref)):
                at = pl.ds(pl.multiple_of(first_row + b * BLOCK, BLOCK) + k * ROWS, ROWS)
                w_ref[at, j : j + LANES] = rows


def decode_kernel(unroll, codes_ref, table_ref, *rest):
    w_ref = rest[-1]
    blocks = codes_ref.shape[1] // ROWS

    def some(i, carry):
        decode_rows(
            i * unroll, unroll, w_ref.shape[1], codes_ref, table_ref, w_ref, i * unroll * BLOCK
        )
        return carry

    lax.fori_loop(0, blocks // unroll, some, 0)


def decode(codes, table, steps, width, into=None, name="decode"):
    _, groups, outputs = codes.shape
    first, count = steps
    operands = [codes, table]
    in_specs = [
        pl.BlockSpec((2, groups, width), lambda n: (0, 0, n + first)),
        pl.BlockSpec(table.shape, lambda n: (0, 0, 0)),
    ]
    aliases = {}
    if into is not None:
        operands.append(into)
        in_specs.append(pl.BlockSpec(memory_space=pl.ANY))
        aliases = {2: 0}
    return pl.pallas_call(
        functools.partial(decode_kernel, min(4, groups // ROWS)),
        grid=(count,),
        in_specs=in_specs,
        out_specs=pl.BlockSpec((groups * GROUP, width), lambda n: (0, n + first)),
        out_shape=jax.ShapeDtypeStruct((groups * GROUP, outputs), jnp.bfloat16),
        input_output_aliases=aliases,
        compiler_params=pltpu.CompilerParams(vmem_limit_bytes=58 * MIB),
        cost_estimate=pl.CostEstimate(
            flops=groups * width * count * 4096,
            bytes_accessed=24 * groups * width * count,
            transcendentals=0,
        ),
        name=name,
    )(*operands)


def order_inputs(orders, me_ref, piece_refs, x_perm, inverse_ref=None, squares_ref=None):
    row = lax.broadcasted_iota(jnp.int32, (LANES, LANES), 0)
    col = lax.broadcasted_iota(jnp.int32, (LANES, LANES), 1)
    source = (col % ROWS) * GROUP + col // ROWS
    swap = jnp.where(row == source, 1.0, 0.0).astype(jnp.bfloat16)
    me = me_ref[0]
    top = 0
    for order, ref in zip(orders, piece_refs):
        _, rows, piece = ref.shape
        squares = jnp.zeros((rows, LANES), jnp.float32)
        for at, relative in enumerate(order):
            for c in range(0, piece, LANES):
                columns = pl.ds(pl.multiple_of((me ^ relative) * piece + c, LANES), LANES)
                values = ref[at, :, c : c + LANES]
                x_perm[top : top + rows, columns] = jnp.dot(
                    values, swap, preferred_element_type=jnp.float32
                ).astype(jnp.bfloat16)
                if squares_ref is not None:
                    plain = values.astype(jnp.float32) * inverse_ref[:, columns]
                    squares = squares + plain * plain
        if squares_ref is not None:
            lane = lax.broadcasted_iota(jnp.int32, (rows, LANES), 1)
            rest = jnp.sum(squares, axis=1, keepdims=True)
            terms = jnp.zeros((rows, LANES), jnp.float32)
            for term in range(3):
                rounded = rest.astype(jnp.bfloat16).astype(jnp.float32)
                terms = jnp.where(lane == term, rounded, terms)
                rest = rest - rounded
            squares_ref[top : top + rows, :] = terms.astype(jnp.bfloat16)
        top += rows


def multiply_kernel(orders, me_ref, *refs):
    count = len(orders)
    piece_refs = refs[:count]
    w_ref, scale_ref, out_ref, x_perm = refs[count:]

    @pl.when(pl.program_id(0) == 0)
    def _():
        order_inputs(orders, me_ref, piece_refs, x_perm)

    product = jnp.dot(x_perm[...], w_ref[...], preferred_element_type=jnp.float32)
    out_ref[...] = (product * scale_ref[...]).astype(out_ref.dtype)


def multiply(gathered, w, scale, steps, width, out_dtype, name):
    orders, pieces, me = gathered
    features, _ = w.shape
    first, count = steps
    batch = sum(p.shape[1] for p in pieces)
    return pl.pallas_call(
        functools.partial(multiply_kernel, orders),
        grid=(count,),
        in_specs=[pl.BlockSpec(memory_space=pltpu.SMEM)]
        + [pl.BlockSpec(p.shape, lambda n: (0, 0, 0)) for p in pieces]
        + [
            pl.BlockSpec((features, width), lambda n: (0, n + first)),
            pl.BlockSpec((1, width), lambda n: (0, n + first)),
        ],
        out_specs=pl.BlockSpec((batch, width), lambda n: (0, n)),
        out_shape=jax.ShapeDtypeStruct((batch, width * count), out_dtype),
        scratch_shapes=[pltpu.VMEM((batch, features), jnp.bfloat16)],
        compiler_params=pltpu.CompilerParams(vmem_limit_bytes=58 * MIB),
        cost_estimate=pl.CostEstimate(
            flops=4 * batch * features * width * count,
            bytes_accessed=2 * features * width * count,
            transcendentals=0,
        ),
        name=name,
    )(me, *pieces, w, scale)


def fused_kernel(orders, chunk, with_squares, me_ref, *refs):
    count = len(orders)
    piece_refs = refs[:count]
    if with_squares:
        inverse_ref, codes_ref, table_ref, scale_ref, out_ref, squares_ref = refs[count : count + 6]
        x_perm, w_even, w_odd, total = refs[count + 6 :]
    else:
        codes_ref, table_ref, scale_ref, out_ref, x_perm, w_even, w_odd, total = refs[count:]
        inverse_ref = squares_ref = None
    features = x_perm.shape[1]
    width = out_ref.shape[1]
    chunks = features // chunk
    blocks = chunk // BLOCK

    @pl.when(pl.program_id(0) == 0)
    def _():
        order_inputs(orders, me_ref, piece_refs, x_perm, inverse_ref, squares_ref)

    def fill(c, w_ref):
        decode_rows(c * blocks, blocks, width, codes_ref, table_ref, w_ref, 0)

    def add(c, w_ref):
        at = pl.ds(pl.multiple_of(c * chunk, chunk), chunk)
        total[...] += jnp.dot(x_perm[:, at], w_ref[...], preferred_element_type=jnp.float32)

    total[...] = jnp.zeros_like(total)
    w_odd[...] = jnp.zeros_like(w_odd)

    def pair(i, carry):
        fill(2 * i, w_even)
        add(jnp.maximum(2 * i - 1, 0), w_odd)
        fill(2 * i + 1, w_odd)
        add(2 * i, w_even)
        return carry

    lax.fori_loop(0, chunks // 2, pair, 0)
    add(chunks - 1, w_odd)
    out_ref[...] = (total[...] * scale_ref[...]).astype(out_ref.dtype)


def fused(gathered, codes, table, scale, steps, width, out_dtype, name, inverse=None):
    orders, pieces, me = gathered
    _, groups, _ = codes.shape
    features = groups * GROUP
    first, count = steps
    batch = sum(p.shape[1] for p in pieces)
    chunk = min(512, features // 2)
    more = [] if inverse is None else [inverse]
    out_specs = [pl.BlockSpec((batch, width), lambda n: (0, n))]
    out_shape = [jax.ShapeDtypeStruct((batch, width * count), out_dtype)]
    if more:
        out_specs.append(pl.BlockSpec((batch, LANES), lambda n: (0, 0)))
        out_shape.append(jax.ShapeDtypeStruct((batch, LANES), jnp.bfloat16))
    return pl.pallas_call(
        functools.partial(fused_kernel, orders, chunk, inverse is not None),
        grid=(count,),
        in_specs=[pl.BlockSpec(memory_space=pltpu.SMEM)]
        + [pl.BlockSpec(p.shape, lambda n: (0, 0, 0)) for p in pieces]
        + [pl.BlockSpec(a.shape, lambda n: (0, 0)) for a in more]
        + [
            pl.BlockSpec((2, groups, width), lambda n: (0, 0, n + first)),
            pl.BlockSpec(table.shape, lambda n: (0, 0, 0)),
            pl.BlockSpec((1, width), lambda n: (0, n + first)),
        ],
        out_specs=out_specs,
        out_shape=out_shape,
        scratch_shapes=[
            pltpu.VMEM((batch, features), jnp.bfloat16),
            pltpu.VMEM((chunk, width), jnp.bfloat16),
            pltpu.VMEM((chunk, width), jnp.bfloat16),
            pltpu.VMEM((batch, width), jnp.float32),
        ],
        compiler_params=pltpu.CompilerParams(vmem_limit_bytes=58 * MIB),
        cost_estimate=pl.CostEstimate(
            flops=groups * width * count * 4096,
            bytes_accessed=8 * groups * width * count,
            transcendentals=0,
        ),
        name=name,
    )(me, *pieces, *more, codes, table, scale)


def exchange(x, move):
    inp, out = lax.axis_size("inp"), lax.axis_size("out")
    pairs = []
    for i in range(inp):
        for o in range(out):
            to_i, to_o = move(i, o)
            pairs.append((i * out + o, to_i * out + to_o))
    return lax.ppermute(x, ("inp", "out"), pairs)


def gather_out(x, cover):
    out = lax.axis_size("out")
    bits = [1 << b for b in range(out.bit_length() - 1)]
    held, order = x[None], [0]
    round_at = 0
    for bit in reversed(bits[2:]):
        (arrived,) = cover(round_at, [exchange(held, lambda i, o: (i, o ^ bit))])
        round_at += 1
        held = jnp.concatenate([held, arrived], axis=0)
        order = order + [r ^ bit for r in order]
    half = x.shape[0] // 2
    halves = [held[:, :half], held[:, half:]]
    orders = [list(order), list(order)]
    ways = [list(reversed(bits[:2])), bits[:2]]
    for step in range(len(bits[:2])):
        arrived = cover(
            round_at,
            [exchange(h, lambda i, o, bit=way[step]: (i, o ^ bit)) for h, way in zip(halves, ways)],
        )
        round_at += 1
        halves = [jnp.concatenate(pair, axis=0) for pair in zip(halves, arrived)]
        orders = [o + [r ^ way[step] for r in o] for o, way in zip(orders, ways)]
    me = lax.axis_index("out").astype(jnp.int32)
    if x.shape[1] % LANES:
        whole = []
        for order, stack in zip(orders, halves):
            place = jnp.array([order.index(r) for r in range(out)], jnp.int32)
            stack = jnp.take(stack, place[me ^ jnp.arange(out, dtype=jnp.int32)], axis=0)
            whole.append(jnp.transpose(stack, (1, 0, 2)).reshape(1, half, out * x.shape[1]))
        orders, halves, me = [[0], [0]], whole, jnp.zeros_like(me)
    return tuple(tuple(o) for o in orders), halves, me[None]


def split_inp(partial, axis):
    inp = lax.axis_size("inp")
    me = lax.axis_index("inp")
    block = partial.shape[axis] // inp
    blocks = [
        lax.dynamic_slice_in_dim(partial, (me ^ d) * block, block, axis) for d in range(inp)
    ]
    return blocks[0], blocks[1:]


def send_inp(blocks):
    return [exchange(b, lambda i, o, d=d: (i ^ d, o)) for d, b in enumerate(blocks, start=1)]


def add_up(terms):
    total = terms[0].astype(jnp.float32)
    for term in terms[1:]:
        total = total + term.astype(jnp.float32)
    return total


def scatter_sum(partial, axis, cover=None):
    kept, leaving = split_inp(partial, axis)
    arrived = send_inp(leaving)
    if cover is not None:
        arrived = cover(arrived)
    return add_up([kept] + arrived)


def gather_inp(x):
    inp = lax.axis_size("inp")
    me = lax.axis_index("inp")
    width = x.shape[1]
    whole = jnp.zeros((x.shape[0], width * inp), x.dtype)
    whole = lax.dynamic_update_slice_in_dim(whole, x, me * width, 1)
    for d in range(1, inp):
        piece = exchange(x, lambda i, o, d=d: (i ^ d, o))
        whole = lax.dynamic_update_slice_in_dim(whole, piece, (me ^ d) * width, 1)
    return whole


class Ahead:
    def __init__(self, codes, table, name):
        self.codes, self.table, self.name = codes, table, name
        self.width = math.gcd(codes.shape[2], 256)
        self.steps = codes.shape[2] // self.width
        self.done = 0
        self.limit = self.steps
        self.buffer = None

    def run(self, count):
        count = min(count, self.limit - self.done)
        if count > 0:
            self.buffer = decode(
                self.codes, self.table, (self.done, count), self.width, self.buffer, self.name
            )
            self.done += count

    def beside(self, count, arrays):
        self.run(count)
        self.buffer, *arrays = lax.optimization_barrier((self.buffer, *arrays))
        return arrays


def per_device(
    attention, residual, wo_codes, wo_books, wo_scale, norm_gain, gate_codes, gate_books, gate_scale
):
    inp = lax.axis_size("inp")
    out = lax.axis_size("out")
    inp_at = lax.axis_index("inp")
    out_at = lax.axis_index("out")
    model = norm_gain.shape[0]
    wo = Ahead(wo_codes, spread_books(wo_books), "decode_wo")
    gate = Ahead(gate_codes, spread_books(gate_books), "decode_gate")
    gate.limit = gate.steps - max(2, gate.steps * 8 // 26)

    features = gather_out(attention, lambda n, arrays: wo.beside(2, arrays))
    wo.run(wo.steps)
    partial = multiply(
        features, wo.buffer, wo_scale[None, :], (0, wo.steps), wo.width, jnp.bfloat16, "multiply_wo"
    )
    summed = scatter_sum(partial, 1, lambda arrays: gate.beside(3, arrays))
    piece = summed.shape[1]
    kept = lax.dynamic_slice_in_dim(residual, inp_at * piece, piece, 1)
    hidden = kept.astype(jnp.float32) + summed
    gain = lax.dynamic_slice_in_dim(norm_gain, (out_at * inp + inp_at) * piece, piece, 0)
    gained = (hidden * gain[None, :]).astype(jnp.bfloat16)

    per_block = out // inp
    (moved,) = gate.beside(
        3, [exchange(gained, lambda q, o: (o // per_block, (o % per_block) * inp + q))]
    )
    gate_in = gather_out(moved, lambda n, arrays: gate.beside(3, arrays))
    stream = gather_inp(hidden.astype(jnp.bfloat16))

    block = model // inp
    inverse = 1.0 / lax.dynamic_slice_in_dim(norm_gain, inp_at * block, block, 0)[None, :]
    scale = gate_scale[None, :]
    orders, pieces, me = gate_in

    def late(steps, gathered, extra=None):
        return fused(
            gathered, gate.codes, gate.table, scale, steps, gate.width, jnp.bfloat16, "fused_gate", extra
        )

    def early(steps, gathered):
        return [
            multiply(gathered, gate.buffer, scale, steps, gate.width, jnp.bfloat16, "multiply_gate")
        ]

    later = gate.steps - gate.done
    jobs = [
        (functools.partial(late, extra=inverse), gate.done, later // 2),
        (late, gate.done + later // 2, later - later // 2),
        (early, 0, gate.done // 2),
        (early, gate.done // 2, gate.done - gate.done // 2),
    ]
    blocks = {}
    waiting = None
    squares = None
    for job, first, count in jobs:
        parts = job((first, count), (orders, pieces, me))
        if waiting is not None:
            at, kept, arrived = waiting
            arrived, parts = lax.optimization_barrier((arrived, parts))
            blocks[at] = [kept] + arrived
        kept, leaving = split_inp(parts[0], 0)
        if len(parts) > 1:
            squares = scatter_sum(parts[1], 0)
        leaving, pieces = lax.optimization_barrier((leaving, pieces))
        waiting = (first, kept, send_inp(leaving))
    at, kept, arrived = waiting
    blocks[at] = [kept] + arrived
    row_factor = lax.rsqrt(jnp.sum(squares, axis=1, keepdims=True) / model + epsilon)
    gate_out = jnp.concatenate(
        [(add_up(blocks[at]) * row_factor).astype(jnp.bfloat16) for at in sorted(blocks)], axis=1
    )
    return (stream, gate_out)


def solution(mesh):
    placed = (
        P(None, ("inp", "out")),
        P(None, "out"),
        P(None, "inp", "out"),
        P(),
        P("out"),
        P(),
        P(None, "inp", "out"),
        P(),
        P("out"),
    )
    return jax.shard_map(
        per_device,
        mesh=mesh,
        in_specs=placed,
        out_specs=(P(None, "out"), P("inp", "out")),
        check_vma=False,
    )
```

```python
import functools
import math

import jax
import jax.numpy as jnp
from jax import lax
from jax.experimental import pallas as pl
from jax.experimental.pallas import tpu as pltpu
from jax.sharding import PartitionSpec as P


epsilon = 1e-05
LANES = 128
GROUP = 8
ROWS = 16
BLOCK = ROWS * GROUP
MIB = 1024 * 1024
UNROLL = 8
EARLY = (5, 4)

take_lanes = lax.GatherDimensionNumbers(
    offset_dims=(),
    collapsed_slice_dims=(1,),
    start_index_map=(1,),
    operand_batching_dims=(0,),
    start_indices_batching_dims=(0,),
)


take_rows = lax.GatherDimensionNumbers(
    offset_dims=(),
    collapsed_slice_dims=(0,),
    start_index_map=(0,),
    operand_batching_dims=(1,),
    start_indices_batching_dims=(1,),
)

BY_LANE = 5
PAIR = 2 * ROWS


def lookup(table, index, dims=take_lanes):
    return lax.gather(
        table,
        index[..., None],
        dims,
        slice_sizes=(1, 1),
        mode=lax.GatherScatterMode.PROMISE_IN_BOUNDS,
    )


def spread_books(books):
    count, entries, group = books.shape
    halves = entries // LANES
    values = books.astype(jnp.float32)
    top = jnp.maximum(jnp.max(jnp.abs(values)), 2.0**-60)
    factor = jnp.float32(1.0)
    for step in (64, 32, 16, 8, 4, 2, 1):
        more = factor * 2.0**step
        factor = jnp.where(top * more <= 224.0, more, factor)
    values = values * factor
    rows = jnp.transpose(values.reshape(count, halves, LANES, group), (0, 1, 3, 2))
    rows = rows.reshape(count * halves * group, 1, LANES).astype(jnp.bfloat16)
    rows = jnp.broadcast_to(rows, (count * halves * group, ROWS, LANES))
    rest = jnp.transpose(values[:, :, BY_LANE:], (2, 0, 1))
    first = rest.astype(jnp.float8_e4m3fn)
    second = ((rest - first.astype(jnp.float32)) * 16.0).astype(jnp.float8_e4m3fn)
    terms = jnp.stack([first, second], axis=2).reshape(-1, PAIR, 1)
    return rows, jnp.broadcast_to(terms, (terms.shape[0], PAIR, LANES)), 1.0 / factor


def decode_block(codes, table_ref, terms):
    rows = [[], []]
    picked = [[], []]
    for half in range(2):
        for book, code in enumerate(codes):
            narrow = code[half * ROWS : (half + 1) * ROWS].astype(jnp.int16)
            low = narrow < LANES
            index = narrow & (LANES - 1)
            first = [lookup(table_ref[(book * 2) * GROUP + k], index) for k in range(BY_LANE)]
            second = [lookup(table_ref[(book * 2 + 1) * GROUP + k], index) for k in range(BY_LANE)]
            picked[book] = [jnp.where(low, a, b) for a, b in zip(first, second)]
        rows[half] = [a + b for a, b in zip(*picked)]
    if BY_LANE == GROUP:
        return rows
    index, bits = [], []
    for code in codes:
        low = (code & (LANES - 1)).astype(jnp.int8)
        high = (code >> 7).astype(jnp.int8)
        index.append(low & (PAIR - 1))
        bits.append([(low & 32) != 0, (low & 64) != 0, high != 0])
    parts = 8
    for k in range(GROUP - BY_LANE):
        sums = []
        for term in range(2):
            total = None
            for book in range(2):
                base = ((k * 2 + book) * 2 + term) * parts
                level = [lookup(terms[base + t], index[book], take_rows) for t in range(parts)]
                for bit in bits[book]:
                    level = [jnp.where(bit, level[n + 1], level[n]) for n in range(0, len(level), 2)]
                value = level[0].astype(jnp.bfloat16)
                total = value if total is None else total + value
            sums.append(total)
        value = sums[0] + sums[1] * jnp.bfloat16(0.0625)
        for half in range(2):
            rows[half].append(value[half * ROWS : (half + 1) * ROWS])
    return rows


def decode_rows(first_pair, pairs, width, codes_ref, table_ref, terms_ref, w_ref, first_row):
    terms = [terms_ref[n] for n in range(terms_ref.shape[0])]
    for b in range(pairs):
        groups = pl.ds(pl.multiple_of((first_pair + b) * PAIR, PAIR), PAIR)
        for j in range(0, width, LANES):
            codes = [codes_ref[book, groups, j : j + LANES] for book in range(2)]
            for half, values in enumerate(decode_block(codes, table_ref, terms)):
                for k, rows in enumerate(values):
                    at = pl.multiple_of(first_row + (2 * b + half) * BLOCK, BLOCK) + k * ROWS
                    w_ref[pl.ds(at, ROWS), j : j + LANES] = rows


def decode_kernel(unroll, codes_ref, table_ref, terms_ref, *rest):
    w_ref = rest[-1]
    pairs = codes_ref.shape[1] // PAIR

    def some(i, carry):
        first = i * unroll
        row = first * 2 * BLOCK
        decode_rows(first, unroll, w_ref.shape[1], codes_ref, table_ref, terms_ref, w_ref, row)
        return carry

    lax.fori_loop(0, pairs // unroll, some, 0)


def decode(codes, tables, steps, width, into=None, name="decode"):
    _, groups, outputs = codes.shape
    first, count = steps
    operands = [codes, *tables]
    in_specs = [
        pl.BlockSpec((2, groups, width), lambda n: (0, 0, n + first)),
        pl.BlockSpec(tables[0].shape, lambda n: (0, 0, 0)),
        pl.BlockSpec(tables[1].shape, lambda n: (0, 0, 0)),
    ]
    aliases = {}
    if into is not None:
        operands.append(into)
        in_specs.append(pl.BlockSpec(memory_space=pl.ANY))
        aliases = {3: 0}
    return pl.pallas_call(
        functools.partial(decode_kernel, min(UNROLL, groups // PAIR)),
        grid=(count,),
        in_specs=in_specs,
        out_specs=pl.BlockSpec((None, groups * GROUP, width), lambda n: (n + first, 0, 0)),
        out_shape=jax.ShapeDtypeStruct((outputs // width, groups * GROUP, width), jnp.bfloat16),
        input_output_aliases=aliases,
        compiler_params=pltpu.CompilerParams(vmem_limit_bytes=58 * MIB),
        cost_estimate=pl.CostEstimate(
            flops=groups * width * count * 8192,
            bytes_accessed=24 * groups * width * count,
            transcendentals=0,
        ),
        name=name,
    )(*operands)


def order_inputs(relatives, me, piece_refs, x_perm, inverse_ref=None, squares_ref=None):
    row = lax.broadcasted_iota(jnp.int32, (LANES, LANES), 0)
    col = lax.broadcasted_iota(jnp.int32, (LANES, LANES), 1)
    source = (col % ROWS) * GROUP + col // ROWS
    swap = jnp.where(row == source, 1.0, 0.0).astype(jnp.bfloat16)
    batch = x_perm.shape[0]
    squares = jnp.zeros((batch, LANES), jnp.float32)
    for relative, ref in zip(relatives, piece_refs):
        piece = ref.shape[1]
        for c in range(0, piece, LANES):
            columns = pl.ds(pl.multiple_of((me ^ relative) * piece + c, LANES), LANES)
            values = ref[:, c : c + LANES]
            x_perm[:, columns] = jnp.dot(values, swap, preferred_element_type=jnp.float32).astype(
                jnp.bfloat16
            )
            if squares_ref is not None:
                plain = values.astype(jnp.float32) * inverse_ref[:, columns]
                squares = squares + plain * plain
    if squares_ref is not None:
        lane = lax.broadcasted_iota(jnp.int32, (batch, LANES), 1)
        rest = jnp.sum(squares, axis=1, keepdims=True)
        terms = jnp.zeros((batch, LANES), jnp.float32)
        for term in range(3):
            rounded = rest.astype(jnp.bfloat16).astype(jnp.float32)
            terms = jnp.where(lane == term, rounded, terms)
            rest = rest - rounded
        squares_ref[...] = terms.astype(jnp.bfloat16)


def multiply_kernel(relatives, with_squares, me_ref, *refs):
    count = len(relatives)
    piece_refs, refs = refs[:count], refs[count:]
    inverse_ref = squares_ref = None
    if with_squares:
        inverse_ref, refs = refs[0], refs[1:]
    w_ref, scale_ref, *out_refs = refs[:-2]
    x_perm, product = refs[-2:]
    if with_squares:
        squares_ref = out_refs.pop()

    @pl.when(pl.program_id(0) == 0)
    def _():
        order_inputs(relatives, me_ref[0], piece_refs, x_perm, inverse_ref, squares_ref)

    product[...] = (
        jnp.dot(x_perm[...], w_ref[...], preferred_element_type=jnp.float32) * scale_ref[...]
    )
    rows = out_refs[0].shape[0]
    for relative, out_ref in enumerate(out_refs):
        first = 0 if len(out_refs) == 1 else pl.multiple_of((me_ref[1] ^ relative) * rows, rows)
        out_ref[...] = product[pl.ds(first, rows), :].astype(out_ref.dtype)


def multiply(gathered, w, scale, steps, width, splits, name, inverse=None):
    relatives, pieces, me = gathered
    _, features, _ = w.shape
    first, count = steps
    batch = pieces[0].shape[0]
    more = [] if inverse is None else [inverse]
    out_specs = [pl.BlockSpec((batch // splits, width), lambda n: (0, n))] * splits
    out_shape = [jax.ShapeDtypeStruct((batch // splits, width * count), jnp.bfloat16)] * splits
    if more:
        out_specs = out_specs + [pl.BlockSpec((batch, LANES), lambda n: (0, 0))]
        out_shape = out_shape + [jax.ShapeDtypeStruct((batch, LANES), jnp.bfloat16)]
    return pl.pallas_call(
        functools.partial(multiply_kernel, relatives, inverse is not None),
        grid=(count,),
        in_specs=[pl.BlockSpec(memory_space=pltpu.SMEM)]
        + [pl.BlockSpec(p.shape, lambda n: (0, 0)) for p in pieces + more]
        + [
            pl.BlockSpec((None, features, width), lambda n: (n + first, 0, 0)),
            pl.BlockSpec((1, width), lambda n: (0, n + first)),
        ],
        out_specs=out_specs,
        out_shape=out_shape,
        scratch_shapes=[
            pltpu.VMEM((batch, features), jnp.bfloat16),
            pltpu.VMEM((batch, width), jnp.float32),
        ],
        compiler_params=pltpu.CompilerParams(vmem_limit_bytes=50 * MIB),
        cost_estimate=pl.CostEstimate(
            flops=4 * batch * features * width * count,
            bytes_accessed=2 * features * width * count,
            transcendentals=0,
        ),
        name=name,
    )(me, *pieces, *more, w, scale)


def exchange(x, move):
    inp, out = lax.axis_size("inp"), lax.axis_size("out")
    pairs = []
    for i in range(inp):
        for o in range(out):
            to_i, to_o = move(i, o)
            pairs.append((i * out + o, to_i * out + to_o))
    return lax.ppermute(x, ("inp", "out"), pairs)


def gather_out(x, move, own):
    out = lax.axis_size("out")
    pieces = [x] if own else []
    for relative in range(len(pieces), out):
        pieces.append(exchange(x, functools.partial(move, relative=relative)))
    return pieces


def whole_rows(pieces):
    out = lax.axis_size("out")
    me = lax.axis_index("out").astype(jnp.int32)
    relatives = tuple(range(out))
    if pieces[0].shape[1] % LANES:
        stack = jnp.take(jnp.stack(pieces), me ^ jnp.arange(out, dtype=jnp.int32), axis=0)
        rows, width = pieces[0].shape
        pieces = [jnp.transpose(stack, (1, 0, 2)).reshape(rows, out * width)]
        relatives, me = (0,), jnp.zeros_like(me)
    return relatives, pieces, jnp.stack([me, lax.axis_index("inp").astype(jnp.int32)])


def split_inp(partial, axis):
    inp = lax.axis_size("inp")
    me = lax.axis_index("inp")
    block = partial.shape[axis] // inp
    blocks = [
        lax.dynamic_slice_in_dim(partial, (me ^ d) * block, block, axis) for d in range(inp)
    ]
    return blocks[0], blocks[1:]


def send_inp(blocks):
    return [exchange(b, lambda i, o, d=d: (i ^ d, o)) for d, b in enumerate(blocks, start=1)]


def add_up(terms):
    total = terms[0].astype(jnp.float32)
    for term in terms[1:]:
        total = total + term.astype(jnp.float32)
    return total


def scatter_sum(partial, axis, cover=None):
    kept, leaving = split_inp(partial, axis)
    arrived = send_inp(leaving)
    if cover is not None:
        arrived = cover(arrived)
    return add_up([kept] + arrived)


def side_by_side(pieces):
    inp = lax.axis_size("inp")
    me = lax.axis_index("inp")
    rows, width = pieces[0].shape
    whole = jnp.zeros((rows, width * inp), pieces[0].dtype)
    for d, piece in enumerate(pieces):
        whole = lax.dynamic_update_slice_in_dim(whole, piece, (me ^ d) * width, 1)
    return whole


class Ahead:
    def __init__(self, codes, books, scale, name):
        *self.tables, factor = spread_books(books)
        self.codes, self.name = codes, name
        self.scale = (scale * factor)[None, :]
        self.width = math.gcd(codes.shape[2], 256)
        self.steps = codes.shape[2] // self.width
        self.done = 0
        self.buffer = None

    def run(self, count):
        count = min(count, self.steps - self.done)
        if count > 0:
            self.buffer = decode(
                self.codes, self.tables, (self.done, count), self.width, self.buffer, self.name
            )
            self.done += count

    def after(self, arrays):
        if self.buffer is None:
            self.codes, *arrays = lax.optimization_barrier((self.codes, *arrays))
        else:
            self.buffer, *arrays = lax.optimization_barrier((self.buffer, *arrays))
        return arrays

    def beside(self, count, arrays):
        self.run(count)
        return self.after(arrays)


def per_device(
    attention, residual, wo_codes, wo_books, wo_scale, norm_gain, gate_codes, gate_books, gate_scale
):
    inp = lax.axis_size("inp")
    out = lax.axis_size("out")
    inp_at = lax.axis_index("inp")
    out_at = lax.axis_index("out")
    model = norm_gain.shape[0]
    wo = Ahead(wo_codes, wo_books, wo_scale, "decode_wo")
    gate = Ahead(gate_codes, gate_books, gate_scale, "decode_gate")
    share = gate.steps / 26

    pieces = gather_out(attention, lambda i, o, relative: (i, o ^ relative), True)
    wo.run(wo.steps)
    gate.codes, wo.buffer = lax.optimization_barrier((gate.codes, wo.buffer))
    pieces = gate.beside(int(EARLY[0] * share), pieces)
    (partial,) = multiply(
        whole_rows(pieces), wo.buffer, wo.scale, (0, wo.steps), wo.width, 1, "multiply_wo"
    )
    kept, leaving = split_inp(partial, 1)
    leaving = gate.after(leaving)
    arrived = gate.beside(int(EARLY[1] * share), send_inp(leaving))
    piece = kept.shape[1]
    own = lax.dynamic_slice_in_dim(residual, inp_at * piece, piece, 1)
    hidden = own.astype(jnp.float32) + add_up([kept] + arrived)
    gain = lax.dynamic_slice_in_dim(norm_gain, (out_at * inp + inp_at) * piece, piece, 0)
    gained = (hidden * gain[None, :]).astype(jnp.bfloat16)
    rounded = hidden.astype(jnp.bfloat16)

    per_block = out // inp
    gained, rounded = gate.after([gained, rounded])
    pieces = gather_out(
        gained,
        lambda q, o, relative: (o // per_block, ((o % per_block) * inp + q) ^ relative),
        False,
    )
    stream_pieces = send_inp([rounded] * (inp - 1))
    arrived = gate.beside(gate.steps, pieces + stream_pieces)
    pieces, stream_pieces = arrived[: len(pieces)], arrived[len(pieces) :]
    stream = side_by_side([rounded] + stream_pieces)

    relatives, pieces, me = whole_rows(pieces)
    block = model // inp
    inverse = 1.0 / lax.dynamic_slice_in_dim(norm_gain, inp_at * block, block, 0)[None, :]
    cuts = [0, gate.steps * 10 // 26, gate.steps * 19 // 26, gate.steps]
    blocks = []
    waiting = None
    squares = None
    for first, last in zip(cuts, cuts[1:]):
        parts = list(multiply(
            (relatives, pieces, me),
            gate.buffer,
            gate.scale,
            (first, last - first),
            gate.width,
            inp,
            "multiply_gate",
            inverse if squares is None else None,
        ))
        if waiting is not None:
            kept, arrived = waiting
            arrived, parts = lax.optimization_barrier((arrived, parts))
            blocks.append([kept] + arrived)
        if squares is None:
            squares = scatter_sum(parts.pop(), 0)
        kept, *leaving = parts
        leaving, pieces = lax.optimization_barrier((leaving, pieces))
        waiting = (kept, send_inp(leaving))
    kept, arrived = waiting
    blocks.append([kept] + arrived)
    row_factor = lax.rsqrt(jnp.sum(squares, axis=1, keepdims=True) / model + epsilon)
    gate_out = jnp.concatenate(
        [(add_up(terms) * row_factor).astype(jnp.bfloat16) for terms in blocks], axis=1
    )
    return (stream, gate_out)


def solution(mesh):
    placed = (
        P(None, ("inp", "out")),
        P(None, "out"),
        P(None, "inp", "out"),
        P(),
        P("out"),
        P(),
        P(None, "inp", "out"),
        P(),
        P("out"),
    )
    return jax.shard_map(
        per_device,
        mesh=mesh,
        in_specs=placed,
        out_specs=(P(None, "out"), P("inp", "out")),
        check_vma=False,
    )
```

```python
import functools
import math

import jax
import jax.numpy as jnp
from jax import lax
from jax.experimental import pallas as pl
from jax.experimental.pallas import tpu as pltpu
from jax.sharding import PartitionSpec as P


epsilon = 1e-05
LANES = 128
GROUP = 8
ROWS = 16
BLOCK = ROWS * GROUP
MIB = 1024 * 1024
UNROLL = 8
SLABS = 4
COVER = (4, 4, 4, 4, 4)

take_lanes = lax.GatherDimensionNumbers(
    offset_dims=(),
    collapsed_slice_dims=(1,),
    start_index_map=(1,),
    operand_batching_dims=(0,),
    start_indices_batching_dims=(0,),
)


take_rows = lax.GatherDimensionNumbers(
    offset_dims=(),
    collapsed_slice_dims=(0,),
    start_index_map=(0,),
    operand_batching_dims=(1,),
    start_indices_batching_dims=(1,),
)

BY_LANE = 5
PAIR = 2 * ROWS


def lookup(table, index, dims=take_lanes):
    return lax.gather(
        table,
        index[..., None],
        dims,
        slice_sizes=(1, 1),
        mode=lax.GatherScatterMode.PROMISE_IN_BOUNDS,
    )


def tables_kernel(*refs):
    count = len(refs) // 4
    for books_ref, lanes_ref, rows_ref, undo_ref in zip(*(refs[n * count : (n + 1) * count] for n in range(4))):
        books, group, entries = books_ref.shape
        values = books_ref[...].astype(jnp.float32)
        top = jnp.max(jnp.abs(values), axis=(0, 1, 2), keepdims=True)[0]
        top = jnp.maximum(top, 2.0**-60)
        factor = jnp.ones_like(top)
        for step in (64, 32, 16, 8, 4, 2, 1):
            more = factor * 2.0**step
            factor = jnp.where(top * more <= 224.0, more, factor)
        undo_ref[...] = jnp.broadcast_to(1.0 / factor, undo_ref.shape)
        row = lax.broadcasted_iota(jnp.int32, (group, LANES), 0)
        for book in range(books):
            scaled = values[book] * factor
            for half in range(entries // LANES):
                at = slice(half * LANES, (half + 1) * LANES)
                for k in range(BY_LANE):
                    lanes_ref[(book * 2 + half) * group + k] = jnp.broadcast_to(
                        scaled[k : k + 1, at], (ROWS, LANES)
                    ).astype(jnp.bfloat16)
            for k in range(BY_LANE, group):
                pick = jnp.where(row == k, 1.0, 0.0).astype(jnp.bfloat16)
                column = lax.dot_general(
                    scaled.astype(jnp.bfloat16), pick, (((0,), (0,)), ((), ())), preferred_element_type=jnp.float32
                )
                first = column.astype(jnp.float8_e4m3fn)
                second = ((column - first.astype(jnp.float32)) * 16.0).astype(jnp.float8_e4m3fn)
                parts = entries // PAIR
                for term, terms in enumerate((first, second)):
                    base = (((k - BY_LANE) * 2 + book) * 2 + term) * parts
                    for part in range(parts):
                        rows_ref[base + part] = terms[part * PAIR : (part + 1) * PAIR]


def make_tables(*all_books):
    turned = [jnp.swapaxes(books, 1, 2) for books in all_books]
    count = len(turned)
    lanes, rows, undo = [], [], []
    for books, group, entries in (t.shape for t in turned):
        lanes.append(jax.ShapeDtypeStruct((books * (entries // LANES) * group, ROWS, LANES), jnp.bfloat16))
        parts = (group - BY_LANE) * books * 2 * (entries // PAIR)
        rows.append(jax.ShapeDtypeStruct((parts, PAIR, LANES), jnp.float8_e4m3fn))
        undo.append(jax.ShapeDtypeStruct((1, LANES), jnp.float32))
    made = pl.pallas_call(tables_kernel, out_shape=lanes + rows + undo, name="make_tables")(*turned)
    return [(made[n], made[count + n], made[2 * count + n]) for n in range(count)]


def decode_block(codes, table_ref, terms):
    rows = [[], []]
    picked = [[], []]
    for half in range(2):
        for book, code in enumerate(codes):
            narrow = code[half * ROWS : (half + 1) * ROWS].astype(jnp.int16)
            low = narrow < LANES
            index = narrow & (LANES - 1)
            first = [lookup(table_ref[(book * 2) * GROUP + k], index) for k in range(BY_LANE)]
            second = [lookup(table_ref[(book * 2 + 1) * GROUP + k], index) for k in range(BY_LANE)]
            picked[book] = [jnp.where(low, a, b) for a, b in zip(first, second)]
        rows[half] = [a + b for a, b in zip(*picked)]
    if BY_LANE == GROUP:
        return rows
    index, bits = [], []
    for code in codes:
        low = (code & (LANES - 1)).astype(jnp.int8)
        high = (code >> 7).astype(jnp.int8)
        index.append(low & (PAIR - 1))
        bits.append([(low & 32) != 0, (low & 64) != 0, high != 0])
    parts = 8
    for k in range(GROUP - BY_LANE):
        sums = []
        for term in range(2):
            total = None
            for book in range(2):
                base = ((k * 2 + book) * 2 + term) * parts
                level = [lookup(terms[base + t], index[book], take_rows) for t in range(parts)]
                for bit in bits[book]:
                    level = [jnp.where(bit, level[n + 1], level[n]) for n in range(0, len(level), 2)]
                value = level[0].astype(jnp.bfloat16)
                total = value if total is None else total + value
            sums.append(total)
        value = sums[0] + sums[1] * jnp.bfloat16(0.0625)
        for half in range(2):
            rows[half].append(value[half * ROWS : (half + 1) * ROWS])
    return rows


def decode_rows(first_pair, pairs, width, codes_ref, table_ref, terms_ref, w_ref, first_row):
    terms = [terms_ref[n] for n in range(terms_ref.shape[0])]
    for b in range(pairs):
        groups = pl.ds(pl.multiple_of((first_pair + b) * PAIR, PAIR), PAIR)
        for j in range(0, width, LANES):
            codes = [codes_ref[book, groups, j : j + LANES] for book in range(2)]
            for half, values in enumerate(decode_block(codes, table_ref, terms)):
                for k, rows in enumerate(values):
                    at = pl.multiple_of(first_row + (2 * b + half) * BLOCK, BLOCK) + k * ROWS
                    w_ref[pl.ds(at, ROWS), j : j + LANES] = rows


def decode_kernel(unroll, codes_ref, table_ref, terms_ref, *rest):
    w_ref = rest[-1]
    pairs = codes_ref.shape[1] // PAIR

    def some(i, carry):
        first = i * unroll
        row = first * 2 * BLOCK
        decode_rows(first, unroll, w_ref.shape[1], codes_ref, table_ref, terms_ref, w_ref, row)
        return carry

    lax.fori_loop(0, pairs // unroll, some, 0)


def decode(codes, tables, steps, width, into=None, name="decode"):
    _, groups, outputs = codes.shape
    first, count = steps
    operands = [codes, *tables]
    in_specs = [
        pl.BlockSpec((2, groups, width), lambda n: (0, 0, n + first)),
        pl.BlockSpec(tables[0].shape, lambda n: (0, 0, 0)),
        pl.BlockSpec(tables[1].shape, lambda n: (0, 0, 0)),
    ]
    aliases = {}
    if into is not None:
        operands.append(into)
        in_specs.append(pl.BlockSpec(memory_space=pl.ANY))
        aliases = {3: 0}
    return pl.pallas_call(
        functools.partial(decode_kernel, min(UNROLL, groups // PAIR)),
        grid=(count,),
        in_specs=in_specs,
        out_specs=pl.BlockSpec((None, groups * GROUP, width), lambda n: (n + first, 0, 0)),
        out_shape=jax.ShapeDtypeStruct((outputs // width, groups * GROUP, width), jnp.bfloat16),
        input_output_aliases=aliases,
        compiler_params=pltpu.CompilerParams(vmem_limit_bytes=58 * MIB),
        cost_estimate=pl.CostEstimate(
            flops=groups * width * count * 8192,
            bytes_accessed=24 * groups * width * count,
            transcendentals=0,
        ),
        name=name,
    )(*operands)


def order_inputs(relatives, me, piece_refs, x_perm, inverse_ref=None, squares_ref=None):
    row = lax.broadcasted_iota(jnp.int32, (LANES, LANES), 0)
    col = lax.broadcasted_iota(jnp.int32, (LANES, LANES), 1)
    source = (col % ROWS) * GROUP + col // ROWS
    swap = jnp.where(row == source, 1.0, 0.0).astype(jnp.bfloat16)
    batch = x_perm.shape[0]
    squares = jnp.zeros((batch, LANES), jnp.float32)
    listed = [(n, ref) for ref in piece_refs for n in range(ref.shape[0])]
    for relative, (n, ref) in zip(relatives, listed):
        piece = ref.shape[2]
        for c in range(0, piece, LANES):
            columns = pl.ds(pl.multiple_of((me ^ relative) * piece + c, LANES), LANES)
            values = ref[n, :, c : c + LANES]
            x_perm[:, columns] = jnp.dot(values, swap, preferred_element_type=jnp.float32).astype(
                jnp.bfloat16
            )
            if squares_ref is not None:
                plain = values.astype(jnp.float32) * inverse_ref[:, columns]
                squares = squares + plain * plain
    if squares_ref is not None:
        lane = lax.broadcasted_iota(jnp.int32, (batch, LANES), 1)
        rest = jnp.sum(squares, axis=1, keepdims=True)
        terms = jnp.zeros((batch, LANES), jnp.float32)
        for term in range(3):
            rounded = rest.astype(jnp.bfloat16).astype(jnp.float32)
            terms = jnp.where(lane == term, rounded, terms)
            rest = rest - rounded
        squares_ref[...] = terms.astype(jnp.bfloat16)


def multiply_kernel(relatives, count, with_squares, me_ref, *refs):
    piece_refs, refs = refs[:count], refs[count:]
    inverse_ref = squares_ref = None
    if with_squares:
        inverse_ref, refs = refs[0], refs[1:]
    w_refs, refs = refs[:SLABS], refs[SLABS:]
    scale_ref, undo_ref, *out_refs = refs[:-2]
    x_perm, product = refs[-2:]
    if with_squares:
        squares_ref = out_refs.pop()

    @pl.when(pl.program_id(0) == 0)
    def _():
        order_inputs(relatives, me_ref[0], piece_refs, x_perm, inverse_ref, squares_ref)

    slab = w_refs[0].shape[0]
    total = sum(
        jnp.dot(x_perm[:, q * slab : (q + 1) * slab], w_ref[...], preferred_element_type=jnp.float32)
        for q, w_ref in enumerate(w_refs)
    )
    product[...] = total * (scale_ref[...] * undo_ref[0:1, 0:1])
    rows = out_refs[0].shape[0]
    for relative, out_ref in enumerate(out_refs):
        first = 0 if len(out_refs) == 1 else pl.multiple_of((me_ref[1] ^ relative) * rows, rows)
        out_ref[...] = product[pl.ds(first, rows), :].astype(out_ref.dtype)


def multiply(gathered, w, scale, undo, steps, width, splits, name, inverse=None):
    relatives, pieces, me = gathered
    _, features, _ = w.shape
    first, count = steps
    batch = pieces[0].shape[1]
    more = [] if inverse is None else [inverse]
    out_specs = [pl.BlockSpec((batch // splits, width), lambda n: (0, n))] * splits
    out_shape = [jax.ShapeDtypeStruct((batch // splits, width * count), jnp.bfloat16)] * splits
    if more:
        out_specs = out_specs + [pl.BlockSpec((batch, LANES), lambda n: (0, 0))]
        out_shape = out_shape + [jax.ShapeDtypeStruct((batch, LANES), jnp.bfloat16)]
    return pl.pallas_call(
        functools.partial(multiply_kernel, relatives, len(pieces), inverse is not None),
        grid=(count,),
        in_specs=[pl.BlockSpec(memory_space=pltpu.SMEM)]
        + [pl.BlockSpec(p.shape, lambda n: (0, 0, 0)) for p in pieces]
        + [pl.BlockSpec(p.shape, lambda n: (0, 0)) for p in more]
        + [
            pl.BlockSpec((None, features // SLABS, width), lambda n, q=q: (n + first, q, 0))
            for q in range(SLABS)
        ]
        + [
            pl.BlockSpec((1, width), lambda n: (0, n + first)),
            pl.BlockSpec(undo.shape, lambda n: (0, 0)),
        ],
        out_specs=out_specs,
        out_shape=out_shape,
        scratch_shapes=[
            pltpu.VMEM((batch, features), jnp.bfloat16),
            pltpu.VMEM((batch, width), jnp.float32),
        ],
        compiler_params=pltpu.CompilerParams(vmem_limit_bytes=50 * MIB),
        cost_estimate=pl.CostEstimate(
            flops=4 * batch * features * width * count,
            bytes_accessed=2 * features * width * count,
            transcendentals=0,
        ),
        name=name,
    )(me, *pieces, *more, *([w] * SLABS), scale, undo)


def exchange(x, move):
    inp, out = lax.axis_size("inp"), lax.axis_size("out")
    pairs = []
    for i in range(inp):
        for o in range(out):
            to_i, to_o = move(i, o)
            pairs.append((i * out + o, to_i * out + to_o))
    return lax.ppermute(x, ("inp", "out"), pairs)


def gather_out(x, cover):
    out = lax.axis_size("out")
    stacks, order = [x[None]], [0]
    for n in range(out.bit_length() - 1):
        bit = out >> (n + 1)
        sent = stacks[0] if n == 0 else jnp.concatenate(stacks)
        (arrived,) = cover(n, [exchange(sent, lambda i, o: (i, o ^ bit))])
        stacks.append(arrived)
        order = order + [r ^ bit for r in order]
    return stacks, order


def whole_rows(stacks, order):
    out = lax.axis_size("out")
    me = lax.axis_index("out").astype(jnp.int32)
    _, rows, width = stacks[0].shape
    if width % LANES:
        place = jnp.array([order.index(r) for r in range(out)], jnp.int32)
        stack = jnp.take(jnp.concatenate(stacks), place[me ^ jnp.arange(out, dtype=jnp.int32)], axis=0)
        stacks = [jnp.transpose(stack, (1, 0, 2)).reshape(1, rows, out * width)]
        order, me = [0], jnp.zeros_like(me)
    return tuple(order), stacks, jnp.stack([me, lax.axis_index("inp").astype(jnp.int32)])


def split_inp(partial, axis):
    inp = lax.axis_size("inp")
    me = lax.axis_index("inp")
    block = partial.shape[axis] // inp
    blocks = [
        lax.dynamic_slice_in_dim(partial, (me ^ d) * block, block, axis) for d in range(inp)
    ]
    return blocks[0], blocks[1:]


def send_inp(blocks):
    return [exchange(b, lambda i, o, d=d: (i ^ d, o)) for d, b in enumerate(blocks, start=1)]


def add_up(terms):
    total = terms[0].astype(jnp.float32)
    for term in terms[1:]:
        total = total + term.astype(jnp.float32)
    return total


def scatter_sum(partial, axis, cover=None):
    kept, leaving = split_inp(partial, axis)
    arrived = send_inp(leaving)
    if cover is not None:
        arrived = cover(arrived)
    return add_up([kept] + arrived)


def side_kernel(order, me_ref, *refs):
    out_ref = refs[-1]
    listed = [(n, ref) for ref in refs[:-1] for n in range(ref.shape[0])]
    for relative, (n, ref) in zip(order, listed):
        width = ref.shape[2]
        at = pl.ds(pl.multiple_of((me_ref[0] ^ relative) * width, LANES), width)
        out_ref[:, at] = ref[n]


def side_by_side(stacks, order):
    inp = lax.axis_size("inp")
    me = lax.axis_index("inp").astype(jnp.int32)
    _, rows, width = stacks[0].shape
    if width % LANES:
        place = jnp.array([order.index(r) for r in range(inp)], jnp.int32)
        stack = jnp.take(jnp.concatenate(stacks), place[me ^ jnp.arange(inp, dtype=jnp.int32)], axis=0)
        return jnp.transpose(stack, (1, 0, 2)).reshape(rows, inp * width)
    return pl.pallas_call(
        functools.partial(side_kernel, tuple(order)),
        in_specs=[pl.BlockSpec(memory_space=pltpu.SMEM)]
        + [pl.BlockSpec(memory_space=pltpu.VMEM)] * len(stacks),
        out_shape=jax.ShapeDtypeStruct((rows, inp * width), stacks[0].dtype),
        name="side_by_side",
    )(me[None], *stacks)


class Ahead:
    def __init__(self, codes, tables, scale, name):
        *self.tables, self.undo = tables
        self.codes, self.name = codes, name
        self.scale = scale[None, :]
        self.width = math.gcd(codes.shape[2], 256)
        self.steps = codes.shape[2] // self.width
        self.done = 0
        self.buffer = None

    def run(self, count):
        count = min(count, self.steps - self.done)
        if count > 0:
            self.buffer = decode(
                self.codes, self.tables, (self.done, count), self.width, self.buffer, self.name
            )
            self.done += count

    def after(self, arrays):
        if self.buffer is None:
            self.codes, *arrays = lax.optimization_barrier((self.codes, *arrays))
        else:
            self.buffer, *arrays = lax.optimization_barrier((self.buffer, *arrays))
        return arrays

    def beside(self, count, arrays):
        self.run(count)
        return self.after(arrays)


def per_device(
    attention, residual, wo_codes, wo_books, wo_scale, norm_gain, gate_codes, gate_books, gate_scale
):
    inp = lax.axis_size("inp")
    out = lax.axis_size("out")
    inp_at = lax.axis_index("inp")
    out_at = lax.axis_index("out")
    model = norm_gain.shape[0]
    wo_tables, gate_tables = make_tables(wo_books, gate_books)
    wo = Ahead(wo_codes, wo_tables, wo_scale, "decode_wo")
    gate = Ahead(gate_codes, gate_tables, gate_scale, "decode_gate")
    share = gate.steps / 26

    def early(n, arrays):
        if n < 2:
            return wo.beside(wo.steps * 3 // 8, arrays)
        wo.run(wo.steps)
        gate.codes, wo.buffer = lax.optimization_barrier((gate.codes, wo.buffer))
        return gate.beside(int(COVER[0] * share), arrays)

    gathered = whole_rows(*gather_out(attention, early))
    (partial,) = multiply(
        gathered, wo.buffer, wo.scale, wo.undo, (0, wo.steps), wo.width, 1, "multiply_wo"
    )
    kept, leaving = split_inp(partial, 1)
    leaving = gate.after(leaving)
    arrived = gate.beside(int(COVER[1] * share), send_inp(leaving))
    piece = kept.shape[1]
    own = lax.dynamic_slice_in_dim(residual, inp_at * piece, piece, 1)
    hidden = own.astype(jnp.float32) + add_up([kept] + arrived)
    gain = lax.dynamic_slice_in_dim(norm_gain, (out_at * inp + inp_at) * piece, piece, 0)
    gained = (hidden * gain[None, :]).astype(jnp.bfloat16)
    rounded = hidden.astype(jnp.bfloat16)

    per_block = out // inp
    gained, rounded = gate.after([gained, rounded])
    (moved,) = gate.beside(
        int(COVER[2] * share),
        [exchange(gained, lambda q, o: (o // per_block, (o % per_block) * inp + q))],
    )
    stream_stacks, stream_order = [rounded[None]], [0]

    def beside_rounds(n, arrays):
        bit = 1 << n
        count = int(COVER[min(3 + n, 4)] * share) if 2 << n < out else gate.steps
        if bit >= inp:
            return gate.beside(count, arrays)
        sent = jnp.concatenate(stream_stacks) if n else stream_stacks[0]
        more = exchange(sent, lambda i, o: (i ^ bit, o))
        arrived, more = gate.beside(count, arrays + [more])
        stream_order.extend([r ^ bit for r in stream_order])
        stream_stacks.append(more)
        return [arrived]

    relatives, stacks, me = whole_rows(*gather_out(moved, beside_rounds))
    stream = side_by_side(stream_stacks, stream_order)

    block = model // inp
    inverse = 1.0 / lax.dynamic_slice_in_dim(norm_gain, inp_at * block, block, 0)[None, :]
    cuts = [0, gate.steps * 10 // 26, gate.steps * 19 // 26, gate.steps]
    blocks = []
    waiting = None
    squares = None
    for first, last in zip(cuts, cuts[1:]):
        parts = list(multiply(
            (relatives, stacks, me),
            gate.buffer,
            gate.scale,
            gate.undo,
            (first, last - first),
            gate.width,
            inp,
            "multiply_gate",
            inverse if squares is None else None,
        ))
        if waiting is not None:
            kept, arrived = waiting
            arrived, parts = lax.optimization_barrier((arrived, parts))
            blocks.append([kept] + arrived)
        if squares is None:
            squares = scatter_sum(parts.pop(), 0)
        kept, *leaving = parts
        leaving, stacks = lax.optimization_barrier((leaving, stacks))
        waiting = (kept, send_inp(leaving))
    kept, arrived = waiting
    blocks.append([kept] + arrived)
    row_factor = lax.rsqrt(jnp.sum(squares, axis=1, keepdims=True) / model + epsilon)
    gate_out = jnp.concatenate(
        [(add_up(terms) * row_factor).astype(jnp.bfloat16) for terms in blocks], axis=1
    )
    return (stream, gate_out)


def solution(mesh):
    placed = (
        P(None, ("inp", "out")),
        P(None, "out"),
        P(None, "inp", "out"),
        P(),
        P("out"),
        P(),
        P(None, "inp", "out"),
        P(),
        P("out"),
    )
    return jax.shard_map(
        per_device,
        mesh=mesh,
        in_specs=placed,
        out_specs=(P(None, "out"), P("inp", "out")),
        check_vma=False,
    )
```

```python
import functools
import math

import jax
import jax.numpy as jnp
from jax import lax
from jax.experimental import pallas as pl
from jax.experimental.pallas import tpu as pltpu
from jax.sharding import PartitionSpec as P


epsilon = 1e-05
LANES = 128
GROUP = 8
ROWS = 16
BLOCK = ROWS * GROUP
MIB = 1024 * 1024
UNROLL = 16
PART = 256
CHUNK = 1024
SLABS = 4
COVER = (2, 2, 2, 2, 2)

take_lanes = lax.GatherDimensionNumbers(
    offset_dims=(),
    collapsed_slice_dims=(1,),
    start_index_map=(1,),
    operand_batching_dims=(0,),
    start_indices_batching_dims=(0,),
)


take_rows = lax.GatherDimensionNumbers(
    offset_dims=(),
    collapsed_slice_dims=(0,),
    start_index_map=(0,),
    operand_batching_dims=(1,),
    start_indices_batching_dims=(1,),
)

BY_LANE = 5
PAIR = 2 * ROWS


def lookup(table, index, dims=take_lanes):
    return lax.gather(
        table,
        index[..., None],
        dims,
        slice_sizes=(1, 1),
        mode=lax.GatherScatterMode.PROMISE_IN_BOUNDS,
    )


def tables_kernel(*refs):
    count = len(refs) // 4
    for books_ref, lanes_ref, rows_ref, undo_ref in zip(*(refs[n * count : (n + 1) * count] for n in range(4))):
        books, group, entries = books_ref.shape
        values = books_ref[...].astype(jnp.float32)
        top = jnp.max(jnp.abs(values), axis=(0, 1, 2), keepdims=True)[0]
        top = jnp.maximum(top, 2.0**-60)
        factor = jnp.ones_like(top)
        for step in (64, 32, 16, 8, 4, 2, 1):
            more = factor * 2.0**step
            factor = jnp.where(top * more <= 224.0, more, factor)
        undo_ref[...] = jnp.broadcast_to(1.0 / factor, undo_ref.shape)
        row = lax.broadcasted_iota(jnp.int32, (group, LANES), 0)
        for book in range(books):
            scaled = values[book] * factor
            for half in range(entries // LANES):
                at = slice(half * LANES, (half + 1) * LANES)
                for k in range(BY_LANE):
                    lanes_ref[(book * 2 + half) * group + k] = jnp.broadcast_to(
                        scaled[k : k + 1, at], (ROWS, LANES)
                    ).astype(jnp.bfloat16)
            for k in range(BY_LANE, group):
                pick = jnp.where(row == k, 1.0, 0.0).astype(jnp.bfloat16)
                column = lax.dot_general(
                    scaled.astype(jnp.bfloat16), pick, (((0,), (0,)), ((), ())), preferred_element_type=jnp.float32
                )
                first = column.astype(jnp.float8_e4m3fn)
                second = ((column - first.astype(jnp.float32)) * 16.0).astype(jnp.float8_e4m3fn)
                parts = entries // PAIR
                for term, terms in enumerate((first, second)):
                    base = (((k - BY_LANE) * 2 + book) * 2 + term) * parts
                    for part in range(parts):
                        rows_ref[base + part] = terms[part * PAIR : (part + 1) * PAIR]


def make_tables(*all_books):
    turned = [jnp.swapaxes(books, 1, 2) for books in all_books]
    count = len(turned)
    lanes, rows, undo = [], [], []
    for books, group, entries in (t.shape for t in turned):
        lanes.append(jax.ShapeDtypeStruct((books * (entries // LANES) * group, ROWS, LANES), jnp.bfloat16))
        parts = (group - BY_LANE) * books * 2 * (entries // PAIR)
        rows.append(jax.ShapeDtypeStruct((parts, PAIR, LANES), jnp.float8_e4m3fn))
        undo.append(jax.ShapeDtypeStruct((1, LANES), jnp.float32))
    made = pl.pallas_call(tables_kernel, out_shape=lanes + rows + undo, name="make_tables")(*turned)
    return [(made[n], made[count + n], made[2 * count + n]) for n in range(count)]


def decode_block(codes, table_ref, terms):
    rows = [[], []]
    picked = [[], []]
    for half in range(2):
        for book, code in enumerate(codes):
            narrow = code[half * ROWS : (half + 1) * ROWS].astype(jnp.int16)
            low = narrow < LANES
            index = narrow & (LANES - 1)
            first = [lookup(table_ref[(book * 2) * GROUP + k], index) for k in range(BY_LANE)]
            second = [lookup(table_ref[(book * 2 + 1) * GROUP + k], index) for k in range(BY_LANE)]
            picked[book] = [jnp.where(low, a, b) for a, b in zip(first, second)]
        rows[half] = [a + b for a, b in zip(*picked)]
    if BY_LANE == GROUP:
        return rows
    index, bits = [], []
    for code in codes:
        low = (code & (LANES - 1)).astype(jnp.int8)
        high = (code >> 7).astype(jnp.int8)
        index.append(low & (PAIR - 1))
        bits.append([(low & 32) != 0, (low & 64) != 0, high != 0])
    parts = 8
    for k in range(GROUP - BY_LANE):
        sums = []
        for term in range(2):
            total = None
            for book in range(2):
                base = ((k * 2 + book) * 2 + term) * parts
                level = [lookup(terms[base + t], index[book], take_rows) for t in range(parts)]
                for bit in bits[book]:
                    level = [jnp.where(bit, level[n + 1], level[n]) for n in range(0, len(level), 2)]
                value = level[0].astype(jnp.bfloat16)
                total = value if total is None else total + value
            sums.append(total)
        value = sums[0] + sums[1] * jnp.bfloat16(0.0625)
        for half in range(2):
            rows[half].append(value[half * ROWS : (half + 1) * ROWS])
    return rows


def decode_rows(first_pair, pairs, width, codes_ref, table_ref, terms_ref, w_ref, first_row):
    terms = [terms_ref[n] for n in range(terms_ref.shape[0])]
    for b in range(pairs):
        groups = pl.ds(pl.multiple_of((first_pair + b) * PAIR, PAIR), PAIR)
        for j in range(0, width, LANES):
            codes = [codes_ref[book, groups, j : j + LANES] for book in range(2)]
            for half, values in enumerate(decode_block(codes, table_ref, terms)):
                for k, rows in enumerate(values):
                    at = pl.multiple_of(first_row + (2 * b + half) * BLOCK, BLOCK) + k * ROWS
                    w_ref[pl.ds(at, ROWS), j : j + LANES] = rows


def decode_kernel(unroll, codes_ref, table_ref, terms_ref, *rest):
    w_ref = rest[-1]
    pairs = codes_ref.shape[1] // PAIR

    def some(i, carry):
        first = i * unroll
        row = first * 2 * BLOCK
        decode_rows(first, unroll, w_ref.shape[1], codes_ref, table_ref, terms_ref, w_ref, row)
        return carry

    lax.fori_loop(0, pairs // unroll, some, 0)


def decode(codes, tables, steps, width, into=None, name="decode"):
    _, groups, outputs = codes.shape
    first, count = steps
    part = math.gcd(width, PART)
    cuts = width // part
    operands = [codes, *tables]
    in_specs = [
        pl.BlockSpec((2, groups, part), lambda n: (0, 0, n + first * cuts)),
        pl.BlockSpec(tables[0].shape, lambda n: (0, 0, 0)),
        pl.BlockSpec(tables[1].shape, lambda n: (0, 0, 0)),
    ]
    aliases = {}
    if into is not None:
        operands.append(into)
        in_specs.append(pl.BlockSpec(memory_space=pl.ANY))
        aliases = {3: 0}
    return pl.pallas_call(
        functools.partial(decode_kernel, min(UNROLL * 128 // part, groups // PAIR)),
        grid=(count * cuts,),
        in_specs=in_specs,
        out_specs=pl.BlockSpec((None, groups * GROUP, part), lambda n: (first + n // cuts, 0, n % cuts)),
        out_shape=jax.ShapeDtypeStruct((outputs // width, groups * GROUP, width), jnp.bfloat16),
        input_output_aliases=aliases,
        compiler_params=pltpu.CompilerParams(vmem_limit_bytes=58 * MIB),
        cost_estimate=pl.CostEstimate(
            flops=groups * width * count * 8192,
            bytes_accessed=24 * groups * width * count,
            transcendentals=0,
        ),
        name=name,
    )(*operands)


def order_inputs(relatives, me, piece_refs, x_perm, inverse_ref=None, squares_ref=None):
    row = lax.broadcasted_iota(jnp.int32, (LANES, LANES), 0)
    col = lax.broadcasted_iota(jnp.int32, (LANES, LANES), 1)
    source = (col % ROWS) * GROUP + col // ROWS
    swap = jnp.where(row == source, 1.0, 0.0).astype(jnp.bfloat16)
    batch = x_perm.shape[0]
    squares = jnp.zeros((batch, LANES), jnp.float32)
    listed = [(n, ref) for ref in piece_refs for n in range(ref.shape[0])]
    for relative, (n, ref) in zip(relatives, listed):
        piece = ref.shape[2]
        for c in range(0, piece, LANES):
            columns = pl.ds(pl.multiple_of((me ^ relative) * piece + c, LANES), LANES)
            values = ref[n, :, c : c + LANES]
            x_perm[:, columns] = jnp.dot(values, swap, preferred_element_type=jnp.float32).astype(
                jnp.bfloat16
            )
            if squares_ref is not None:
                plain = values.astype(jnp.float32) * inverse_ref[:, columns]
                squares = squares + plain * plain
    if squares_ref is not None:
        lane = lax.broadcasted_iota(jnp.int32, (batch, LANES), 1)
        rest = jnp.sum(squares, axis=1, keepdims=True)
        terms = jnp.zeros((batch, LANES), jnp.float32)
        for term in range(3):
            rounded = rest.astype(jnp.bfloat16).astype(jnp.float32)
            terms = jnp.where(lane == term, rounded, terms)
            rest = rest - rounded
        squares_ref[...] = terms.astype(jnp.bfloat16)


def multiply_kernel(relatives, count, with_squares, me_ref, *refs):
    piece_refs, refs = refs[:count], refs[count:]
    inverse_ref = squares_ref = None
    if with_squares:
        inverse_ref, refs = refs[0], refs[1:]
    w_refs, refs = refs[:SLABS], refs[SLABS:]
    scale_ref, undo_ref, *out_refs = refs[:-2]
    x_perm, product = refs[-2:]
    if with_squares:
        squares_ref = out_refs.pop()

    @pl.when(pl.program_id(0) == 0)
    def _():
        order_inputs(relatives, me_ref[0], piece_refs, x_perm, inverse_ref, squares_ref)

    slab = w_refs[0].shape[0]
    total = sum(
        jnp.dot(x_perm[:, q * slab : (q + 1) * slab], w_ref[...], preferred_element_type=jnp.float32)
        for q, w_ref in enumerate(w_refs)
    )
    product[...] = total * (scale_ref[...] * undo_ref[0:1, 0:1])
    rows = out_refs[0].shape[0]
    for relative, out_ref in enumerate(out_refs):
        first = 0 if len(out_refs) == 1 else pl.multiple_of((me_ref[1] ^ relative) * rows, rows)
        out_ref[...] = product[pl.ds(first, rows), :].astype(out_ref.dtype)


def multiply(gathered, w, scale, undo, steps, width, splits, name, inverse=None):
    relatives, pieces, me = gathered
    _, features, _ = w.shape
    first, count = steps
    batch = pieces[0].shape[1]
    more = [] if inverse is None else [inverse]
    out_specs = [pl.BlockSpec((batch // splits, width), lambda n: (0, n))] * splits
    out_shape = [jax.ShapeDtypeStruct((batch // splits, width * count), jnp.bfloat16)] * splits
    if more:
        out_specs = out_specs + [pl.BlockSpec((batch, LANES), lambda n: (0, 0))]
        out_shape = out_shape + [jax.ShapeDtypeStruct((batch, LANES), jnp.bfloat16)]
    return pl.pallas_call(
        functools.partial(multiply_kernel, relatives, len(pieces), inverse is not None),
        grid=(count,),
        in_specs=[pl.BlockSpec(memory_space=pltpu.SMEM)]
        + [pl.BlockSpec(p.shape, lambda n: (0, 0, 0)) for p in pieces]
        + [pl.BlockSpec(p.shape, lambda n: (0, 0)) for p in more]
        + [
            pl.BlockSpec((None, features // SLABS, width), lambda n, q=q: (n + first, q, 0))
            for q in range(SLABS)
        ]
        + [
            pl.BlockSpec((1, width), lambda n: (0, n + first)),
            pl.BlockSpec(undo.shape, lambda n: (0, 0)),
        ],
        out_specs=out_specs,
        out_shape=out_shape,
        scratch_shapes=[
            pltpu.VMEM((batch, features), jnp.bfloat16),
            pltpu.VMEM((batch, width), jnp.float32),
        ],
        compiler_params=pltpu.CompilerParams(vmem_limit_bytes=50 * MIB),
        cost_estimate=pl.CostEstimate(
            flops=4 * batch * features * width * count,
            bytes_accessed=2 * features * width * count,
            transcendentals=0,
        ),
        name=name,
    )(me, *pieces, *more, *([w] * SLABS), scale, undo)


def late_kernel(relatives, count, with_squares, chunk, me_ref, *refs):
    piece_refs, refs = refs[:count], refs[count:]
    inverse_ref = squares_ref = None
    if with_squares:
        inverse_ref, refs = refs[0], refs[1:]
    codes_ref, table_ref, terms_ref, w_ref, now_scale_ref, old_scale_ref, undo_ref, *out_refs = refs[:-5]
    x_perm, w_even, w_odd, old_total, now_total = refs[-5:]
    if with_squares:
        squares_ref = out_refs.pop()
    features = x_perm.shape[1]
    width = w_ref.shape[1]
    chunks = features // chunk
    pairs = chunk // (2 * BLOCK)

    @pl.when(pl.program_id(0) == 0)
    def _():
        order_inputs(relatives, me_ref[0], piece_refs, x_perm, inverse_ref, squares_ref)

    def fill(c, into_ref):
        decode_rows(c * pairs, pairs, width, codes_ref, table_ref, terms_ref, into_ref, 0)

    def rows_of(c):
        return pl.ds(pl.multiple_of(c * chunk, chunk), chunk)

    def add(c, from_ref):
        now_total[...] += jnp.dot(x_perm[:, rows_of(c)], from_ref[...], preferred_element_type=jnp.float32)

    def add_old(c):
        old_total[...] += jnp.dot(
            x_perm[:, rows_of(c)], w_ref[rows_of(c), :], preferred_element_type=jnp.float32
        )

    now_total[...] = jnp.zeros_like(now_total)
    old_total[...] = jnp.zeros_like(old_total)
    w_odd[...] = jnp.zeros_like(w_odd)

    def pair(i, carry):
        fill(2 * i, w_even)
        add(jnp.maximum(2 * i - 1, 0), w_odd)
        add_old(2 * i)
        fill(2 * i + 1, w_odd)
        add(2 * i, w_even)
        add_old(2 * i + 1)
        return carry

    lax.fori_loop(0, chunks // 2, pair, 0)
    add(chunks - 1, w_odd)
    undo = undo_ref[0:1, 0:1]
    old_total[...] = old_total[...] * (old_scale_ref[...] * undo)
    now_total[...] = now_total[...] * (now_scale_ref[...] * undo)
    rows = out_refs[0].shape[1]
    for relative, out_ref in enumerate(out_refs):
        first = pl.multiple_of((me_ref[1] ^ relative) * rows, rows)
        out_ref[0] = old_total[pl.ds(first, rows), :].astype(out_ref.dtype)
        out_ref[1] = now_total[pl.ds(first, rows), :].astype(out_ref.dtype)


def late(gathered, codes, tables, w, scale, undo, now, old, count, width, splits, name, inverse=None):
    relatives, pieces, me = gathered
    _, features, _ = w.shape
    batch = pieces[0].shape[1]
    more = [] if inverse is None else [inverse]
    chunk = min(CHUNK, features // 2)
    rows = batch // splits
    out_specs = [pl.BlockSpec((2, rows, width), lambda n: (0, 0, n))] * splits
    out_shape = [jax.ShapeDtypeStruct((2, rows, width * count), jnp.bfloat16)] * splits
    if more:
        out_specs = out_specs + [pl.BlockSpec((batch, LANES), lambda n: (0, 0))]
        out_shape = out_shape + [jax.ShapeDtypeStruct((batch, LANES), jnp.bfloat16)]
    return pl.pallas_call(
        functools.partial(late_kernel, relatives, len(pieces), inverse is not None, chunk),
        grid=(count,),
        in_specs=[pl.BlockSpec(memory_space=pltpu.SMEM)]
        + [pl.BlockSpec(p.shape, lambda n: (0, 0, 0)) for p in pieces]
        + [pl.BlockSpec(p.shape, lambda n: (0, 0)) for p in more]
        + [
            pl.BlockSpec((2, features // GROUP, width), lambda n: (0, 0, n + now)),
            pl.BlockSpec(tables[0].shape, lambda n: (0, 0, 0)),
            pl.BlockSpec(tables[1].shape, lambda n: (0, 0, 0)),
            pl.BlockSpec((None, features, width), lambda n: (n + old, 0, 0)),
            pl.BlockSpec((1, width), lambda n: (0, n + now)),
            pl.BlockSpec((1, width), lambda n: (0, n + old)),
            pl.BlockSpec(undo.shape, lambda n: (0, 0)),
        ],
        out_specs=out_specs,
        out_shape=out_shape,
        scratch_shapes=[
            pltpu.VMEM((batch, features), jnp.bfloat16),
            pltpu.VMEM((chunk, width), jnp.bfloat16),
            pltpu.VMEM((chunk, width), jnp.bfloat16),
            pltpu.VMEM((batch, width), jnp.float32),
            pltpu.VMEM((batch, width), jnp.float32),
        ],
        compiler_params=pltpu.CompilerParams(vmem_limit_bytes=50 * MIB),
        cost_estimate=pl.CostEstimate(
            flops=features * width * count * 1024,
            bytes_accessed=3 * features * width * count,
            transcendentals=0,
        ),
        name=name,
    )(me, *pieces, *more, codes, *tables, w, scale, scale, undo)


def exchange(x, move):
    inp, out = lax.axis_size("inp"), lax.axis_size("out")
    pairs = []
    for i in range(inp):
        for o in range(out):
            to_i, to_o = move(i, o)
            pairs.append((i * out + o, to_i * out + to_o))
    return lax.ppermute(x, ("inp", "out"), pairs)


def gather_out(x, cover):
    out = lax.axis_size("out")
    stacks, order = [x[None]], [0]
    for n in range(out.bit_length() - 1):
        bit = out >> (n + 1)
        sent = stacks[0] if n == 0 else jnp.concatenate(stacks)
        (arrived,) = cover(n, [exchange(sent, lambda i, o: (i, o ^ bit))])
        stacks.append(arrived)
        order = order + [r ^ bit for r in order]
    return stacks, order


def whole_rows(stacks, order):
    out = lax.axis_size("out")
    me = lax.axis_index("out").astype(jnp.int32)
    _, rows, width = stacks[0].shape
    if width % LANES:
        place = jnp.array([order.index(r) for r in range(out)], jnp.int32)
        stack = jnp.take(jnp.concatenate(stacks), place[me ^ jnp.arange(out, dtype=jnp.int32)], axis=0)
        stacks = [jnp.transpose(stack, (1, 0, 2)).reshape(1, rows, out * width)]
        order, me = [0], jnp.zeros_like(me)
    return tuple(order), stacks, jnp.stack([me, lax.axis_index("inp").astype(jnp.int32)])


def split_inp(partial, axis):
    inp = lax.axis_size("inp")
    me = lax.axis_index("inp")
    block = partial.shape[axis] // inp
    blocks = [
        lax.dynamic_slice_in_dim(partial, (me ^ d) * block, block, axis) for d in range(inp)
    ]
    return blocks[0], blocks[1:]


def send_inp(blocks):
    return [exchange(b, lambda i, o, d=d: (i ^ d, o)) for d, b in enumerate(blocks, start=1)]


def add_up(terms):
    total = terms[0].astype(jnp.float32)
    for term in terms[1:]:
        total = total + term.astype(jnp.float32)
    return total


def scatter_sum(partial, axis, cover=None):
    kept, leaving = split_inp(partial, axis)
    arrived = send_inp(leaving)
    if cover is not None:
        arrived = cover(arrived)
    return add_up([kept] + arrived)


def side_kernel(order, me_ref, *refs):
    out_ref = refs[-1]
    listed = [(n, ref) for ref in refs[:-1] for n in range(ref.shape[0])]
    for relative, (n, ref) in zip(order, listed):
        width = ref.shape[2]
        at = pl.ds(pl.multiple_of((me_ref[0] ^ relative) * width, LANES), width)
        out_ref[:, at] = ref[n]


def side_by_side(stacks, order):
    inp = lax.axis_size("inp")
    me = lax.axis_index("inp").astype(jnp.int32)
    _, rows, width = stacks[0].shape
    if width % LANES:
        place = jnp.array([order.index(r) for r in range(inp)], jnp.int32)
        stack = jnp.take(jnp.concatenate(stacks), place[me ^ jnp.arange(inp, dtype=jnp.int32)], axis=0)
        return jnp.transpose(stack, (1, 0, 2)).reshape(rows, inp * width)
    return pl.pallas_call(
        functools.partial(side_kernel, tuple(order)),
        in_specs=[pl.BlockSpec(memory_space=pltpu.SMEM)]
        + [pl.BlockSpec(memory_space=pltpu.VMEM)] * len(stacks),
        out_shape=jax.ShapeDtypeStruct((rows, inp * width), stacks[0].dtype),
        name="side_by_side",
    )(me[None], *stacks)


def finish_kernel(inp, spans, model, *refs):
    out_ref, refs = refs[-1], refs[:-1]
    terms = sum(ref[...].astype(jnp.float32) for ref in refs[:inp])
    factor = lax.rsqrt(jnp.sum(terms, axis=1, keepdims=True) / model + epsilon)
    for n, starts in enumerate(spans):
        parts = refs[(n + 1) * inp : (n + 2) * inp]
        for half, start in enumerate(starts):
            at = half if len(parts[0].shape) == 3 else slice(None)
            total = sum(part[at].astype(jnp.float32) for part in parts)
            out_ref[:, start : start + total.shape[1]] = (total * factor).astype(jnp.bfloat16)


def finish(squares, blocks, spans, outputs, model):
    operands = list(squares)
    for block in blocks:
        operands += block
    return pl.pallas_call(
        functools.partial(finish_kernel, len(squares), tuple(spans), model),
        in_specs=[pl.BlockSpec(memory_space=pltpu.VMEM)] * len(operands),
        out_shape=jax.ShapeDtypeStruct((squares[0].shape[0], outputs), jnp.bfloat16),
        compiler_params=pltpu.CompilerParams(vmem_limit_bytes=16 * MIB),
        name="finish",
    )(*operands)


class Ahead:
    def __init__(self, codes, tables, scale, name):
        *self.tables, self.undo = tables
        self.codes, self.name = codes, name
        self.scale = scale[None, :]
        self.width = math.gcd(codes.shape[2], 256)
        self.steps = codes.shape[2] // self.width
        self.done = 0
        self.limit = self.steps
        self.buffer = None

    def run(self, count):
        count = min(count, self.limit - self.done)
        if count > 0:
            self.buffer = decode(
                self.codes, self.tables, (self.done, count), self.width, self.buffer, self.name
            )
            self.done += count

    def after(self, arrays):
        if self.buffer is None:
            self.codes, *arrays = lax.optimization_barrier((self.codes, *arrays))
        else:
            self.buffer, *arrays = lax.optimization_barrier((self.buffer, *arrays))
        return arrays

    def beside(self, count, arrays):
        self.run(count)
        return self.after(arrays)


def per_device(
    attention, residual, wo_codes, wo_books, wo_scale, norm_gain, gate_codes, gate_books, gate_scale
):
    inp = lax.axis_size("inp")
    out = lax.axis_size("out")
    inp_at = lax.axis_index("inp")
    out_at = lax.axis_index("out")
    model = norm_gain.shape[0]
    wo_tables, gate_tables = make_tables(wo_books, gate_books)
    wo = Ahead(wo_codes, wo_tables, wo_scale, "decode_wo")
    gate = Ahead(gate_codes, gate_tables, gate_scale, "decode_gate")
    share = gate.steps / 26
    gate.limit = (gate.steps + 1) // 2

    def early(n, arrays):
        if n < 2:
            return wo.beside(wo.steps * 3 // 8, arrays)
        wo.run(wo.steps)
        gate.codes, wo.buffer = lax.optimization_barrier((gate.codes, wo.buffer))
        return gate.beside(int(COVER[0] * share), arrays)

    gathered = whole_rows(*gather_out(attention, early))
    (partial,) = multiply(
        gathered, wo.buffer, wo.scale, wo.undo, (0, wo.steps), wo.width, 1, "multiply_wo"
    )
    kept, leaving = split_inp(partial, 1)
    leaving = gate.after(leaving)
    arrived = gate.beside(int(COVER[1] * share), send_inp(leaving))
    piece = kept.shape[1]
    own = lax.dynamic_slice_in_dim(residual, inp_at * piece, piece, 1)
    hidden = own.astype(jnp.float32) + add_up([kept] + arrived)
    gain = lax.dynamic_slice_in_dim(norm_gain, (out_at * inp + inp_at) * piece, piece, 0)
    gained = (hidden * gain[None, :]).astype(jnp.bfloat16)
    rounded = hidden.astype(jnp.bfloat16)

    per_block = out // inp
    gained, rounded = gate.after([gained, rounded])
    (moved,) = gate.beside(
        int(COVER[2] * share),
        [exchange(gained, lambda q, o: (o // per_block, (o % per_block) * inp + q))],
    )
    stream_stacks, stream_order = [rounded[None]], [0]

    def beside_rounds(n, arrays):
        bit = 1 << n
        count = int(COVER[min(3 + n, 4)] * share) if 2 << n < out else gate.steps
        if bit >= inp:
            return gate.beside(count, arrays)
        sent = jnp.concatenate(stream_stacks) if n else stream_stacks[0]
        more = exchange(sent, lambda i, o: (i ^ bit, o))
        arrived, more = gate.beside(count, arrays + [more])
        stream_order.extend([r ^ bit for r in stream_order])
        stream_stacks.append(more)
        return [arrived]

    relatives, stacks, me = whole_rows(*gather_out(moved, beside_rounds))
    stream = side_by_side(stream_stacks, stream_order)

    block = model // inp
    inverse = 1.0 / lax.dynamic_slice_in_dim(norm_gain, inp_at * block, block, 0)[None, :]
    pairs = gate.steps - gate.done
    single = gate.done - pairs
    jobs = [(0, single)] if single else []
    start = single
    for count in (pairs * 5 // 13, pairs * 5 // 13, pairs - 2 * (pairs * 5 // 13)):
        jobs.append((start, count))
        start += count
    blocks = []
    waiting = None
    squares = None
    for first, count in jobs:
        given = (relatives, stacks, me)
        extra = inverse if squares is None else None
        if first < single:
            parts = multiply(
                given, gate.buffer, gate.scale, gate.undo, (first, count), gate.width, inp, "multiply_gate", extra
            )
        else:
            parts = late(
                given,
                gate.codes,
                gate.tables,
                gate.buffer,
                gate.scale,
                gate.undo,
                gate.done + first - single,
                first,
                count,
                gate.width,
                inp,
                "late_gate",
                extra,
            )
        parts = list(parts)
        if waiting is not None:
            kept, arrived = waiting
            arrived, parts = lax.optimization_barrier((arrived, parts))
            blocks.append([kept] + arrived)
        if squares is None:
            kept, leaving = split_inp(parts.pop(), 0)
            squares = [kept] + send_inp(leaving)
        kept, *leaving = parts
        leaving, stacks = lax.optimization_barrier((leaving, stacks))
        waiting = (kept, send_inp(leaving))
    kept, arrived = waiting
    blocks.append([kept] + arrived)
    width = gate.width
    spans = [
        (first * width,) if first < single else (first * width, (gate.done + first - single) * width)
        for first, _ in jobs
    ]
    gate_out = finish(squares, blocks, spans, gate.steps * width, model)
    return (stream, gate_out)


def solution(mesh):
    placed = (
        P(None, ("inp", "out")),
        P(None, "out"),
        P(None, "inp", "out"),
        P(),
        P("out"),
        P(),
        P(None, "inp", "out"),
        P(),
        P("out"),
    )
    return jax.shard_map(
        per_device,
        mesh=mesh,
        in_specs=placed,
        out_specs=(P(None, "out"), P("inp", "out")),
        check_vma=False,
    )
```

```python
import functools
import math

import jax
import jax.numpy as jnp
from jax import lax
from jax.experimental import pallas as pl
from jax.experimental.pallas import tpu as pltpu
from jax.sharding import PartitionSpec as P


epsilon = 1e-05
LANES = 128
GROUP = 8
ROWS = 16
BLOCK = ROWS * GROUP
MIB = 1024 * 1024
UNROLL = 16
PART = 256
CHUNK = 1024
SLABS = 4
COVER = (2, 2, 2, 2, 2)

take_lanes = lax.GatherDimensionNumbers(
    offset_dims=(),
    collapsed_slice_dims=(1,),
    start_index_map=(1,),
    operand_batching_dims=(0,),
    start_indices_batching_dims=(0,),
)


take_rows = lax.GatherDimensionNumbers(
    offset_dims=(),
    collapsed_slice_dims=(0,),
    start_index_map=(0,),
    operand_batching_dims=(1,),
    start_indices_batching_dims=(1,),
)

BY_LANE = 5
PAIR = 2 * ROWS


def lookup(table, index, dims=take_lanes):
    return lax.gather(
        table,
        index[..., None],
        dims,
        slice_sizes=(1, 1),
        mode=lax.GatherScatterMode.PROMISE_IN_BOUNDS,
    )


def tables_kernel(*refs):
    count = len(refs) // 4
    for books_ref, lanes_ref, rows_ref, undo_ref in zip(*(refs[n * count : (n + 1) * count] for n in range(4))):
        books, group, entries = books_ref.shape
        values = books_ref[...].astype(jnp.float32)
        top = jnp.max(jnp.abs(values), axis=(0, 1, 2), keepdims=True)[0]
        top = jnp.maximum(top, 2.0**-60)
        factor = jnp.ones_like(top)
        for step in (64, 32, 16, 8, 4, 2, 1):
            more = factor * 2.0**step
            factor = jnp.where(top * more <= 224.0, more, factor)
        undo_ref[...] = jnp.broadcast_to(1.0 / factor, undo_ref.shape)
        row = lax.broadcasted_iota(jnp.int32, (group, LANES), 0)
        for book in range(books):
            scaled = values[book] * factor
            for half in range(entries // LANES):
                at = slice(half * LANES, (half + 1) * LANES)
                for k in range(BY_LANE):
                    lanes_ref[(book * 2 + half) * group + k] = jnp.broadcast_to(
                        scaled[k : k + 1, at], (ROWS, LANES)
                    ).astype(jnp.bfloat16)
            for k in range(BY_LANE, group):
                pick = jnp.where(row == k, 1.0, 0.0).astype(jnp.bfloat16)
                column = lax.dot_general(
                    scaled.astype(jnp.bfloat16), pick, (((0,), (0,)), ((), ())), preferred_element_type=jnp.float32
                )
                first = column.astype(jnp.float8_e4m3fn)
                second = ((column - first.astype(jnp.float32)) * 16.0).astype(jnp.float8_e4m3fn)
                parts = entries // PAIR
                for term, terms in enumerate((first, second)):
                    base = (((k - BY_LANE) * 2 + book) * 2 + term) * parts
                    for part in range(parts):
                        rows_ref[base + part] = terms[part * PAIR : (part + 1) * PAIR]


def make_tables(*all_books):
    turned = [jnp.swapaxes(books, 1, 2) for books in all_books]
    count = len(turned)
    lanes, rows, undo = [], [], []
    for books, group, entries in (t.shape for t in turned):
        lanes.append(jax.ShapeDtypeStruct((books * (entries // LANES) * group, ROWS, LANES), jnp.bfloat16))
        parts = (group - BY_LANE) * books * 2 * (entries // PAIR)
        rows.append(jax.ShapeDtypeStruct((parts, PAIR, LANES), jnp.float8_e4m3fn))
        undo.append(jax.ShapeDtypeStruct((1, LANES), jnp.float32))
    made = pl.pallas_call(tables_kernel, out_shape=lanes + rows + undo, name="make_tables")(*turned)
    return [(made[n], made[count + n], made[2 * count + n]) for n in range(count)]


def decode_block(codes, table_ref, terms):
    rows = [[], []]
    picked = [[], []]
    for half in range(2):
        for book, code in enumerate(codes):
            narrow = code[half * ROWS : (half + 1) * ROWS].astype(jnp.int16)
            low = narrow < LANES
            index = narrow & (LANES - 1)
            first = [lookup(table_ref[(book * 2) * GROUP + k], index) for k in range(BY_LANE)]
            second = [lookup(table_ref[(book * 2 + 1) * GROUP + k], index) for k in range(BY_LANE)]
            picked[book] = [jnp.where(low, a, b) for a, b in zip(first, second)]
        rows[half] = [a + b for a, b in zip(*picked)]
    if BY_LANE == GROUP:
        return rows
    index, bits = [], []
    for code in codes:
        low = (code & (LANES - 1)).astype(jnp.int8)
        high = (code >> 7).astype(jnp.int8)
        index.append(low & (PAIR - 1))
        bits.append([(low & 32) != 0, (low & 64) != 0, high != 0])
    parts = 8
    for k in range(GROUP - BY_LANE):
        sums = []
        for term in range(2):
            total = None
            for book in range(2):
                base = ((k * 2 + book) * 2 + term) * parts
                level = [lookup(terms[base + t], index[book], take_rows) for t in range(parts)]
                for bit in bits[book]:
                    level = [jnp.where(bit, level[n + 1], level[n]) for n in range(0, len(level), 2)]
                value = level[0].astype(jnp.bfloat16)
                total = value if total is None else total + value
            sums.append(total)
        value = sums[0] + sums[1] * jnp.bfloat16(0.0625)
        for half in range(2):
            rows[half].append(value[half * ROWS : (half + 1) * ROWS])
    return rows


def decode_rows(first_pair, pairs, width, codes_ref, table_ref, terms_ref, w_ref, first_row):
    terms = [terms_ref[n] for n in range(terms_ref.shape[0])]
    for b in range(pairs):
        groups = pl.ds(pl.multiple_of((first_pair + b) * PAIR, PAIR), PAIR)
        for j in range(0, width, LANES):
            codes = [codes_ref[book, groups, j : j + LANES] for book in range(2)]
            for half, values in enumerate(decode_block(codes, table_ref, terms)):
                for k, rows in enumerate(values):
                    at = pl.multiple_of(first_row + (2 * b + half) * BLOCK, BLOCK) + k * ROWS
                    w_ref[pl.ds(at, ROWS), j : j + LANES] = rows


def decode_kernel(unroll, codes_ref, table_ref, terms_ref, *rest):
    w_ref = rest[-1]
    pairs = codes_ref.shape[1] // PAIR

    def some(i, carry):
        first = i * unroll
        row = first * 2 * BLOCK
        decode_rows(first, unroll, w_ref.shape[1], codes_ref, table_ref, terms_ref, w_ref, row)
        return carry

    lax.fori_loop(0, pairs // unroll, some, 0)


def decode(codes, tables, steps, width, into=None, name="decode"):
    _, groups, outputs = codes.shape
    first, count = steps
    part = math.gcd(width, PART)
    cuts = width // part
    operands = [codes, *tables]
    in_specs = [
        pl.BlockSpec((2, groups, part), lambda n: (0, 0, n + first * cuts)),
        pl.BlockSpec(tables[0].shape, lambda n: (0, 0, 0)),
        pl.BlockSpec(tables[1].shape, lambda n: (0, 0, 0)),
    ]
    aliases = {}
    if into is not None:
        operands.append(into)
        in_specs.append(pl.BlockSpec(memory_space=pl.ANY))
        aliases = {3: 0}
    return pl.pallas_call(
        functools.partial(decode_kernel, min(UNROLL * 128 // part, groups // PAIR)),
        grid=(count * cuts,),
        in_specs=in_specs,
        out_specs=pl.BlockSpec((None, groups * GROUP, part), lambda n: (first + n // cuts, 0, n % cuts)),
        out_shape=jax.ShapeDtypeStruct((outputs // width, groups * GROUP, width), jnp.bfloat16),
        input_output_aliases=aliases,
        compiler_params=pltpu.CompilerParams(vmem_limit_bytes=58 * MIB),
        cost_estimate=pl.CostEstimate(
            flops=groups * width * count * 8192,
            bytes_accessed=24 * groups * width * count,
            transcendentals=0,
        ),
        name=name,
    )(*operands)


def order_inputs(relatives, me, piece_refs, x_perm, inverse_ref=None, squares_ref=None):
    row = lax.broadcasted_iota(jnp.int32, (LANES, LANES), 0)
    col = lax.broadcasted_iota(jnp.int32, (LANES, LANES), 1)
    source = (col % ROWS) * GROUP + col // ROWS
    swap = jnp.where(row == source, 1.0, 0.0).astype(jnp.bfloat16)
    batch = x_perm.shape[0]
    squares = jnp.zeros((batch, LANES), jnp.float32)
    listed = [(n, ref) for ref in piece_refs for n in range(ref.shape[0])]
    for relative, (n, ref) in zip(relatives, listed):
        piece = ref.shape[2]
        for c in range(0, piece, LANES):
            columns = pl.ds(pl.multiple_of((me ^ relative) * piece + c, LANES), LANES)
            values = ref[n, :, c : c + LANES]
            x_perm[:, columns] = jnp.dot(values, swap, preferred_element_type=jnp.float32).astype(
                jnp.bfloat16
            )
            if squares_ref is not None:
                plain = values.astype(jnp.float32) * inverse_ref[:, columns]
                squares = squares + plain * plain
    if squares_ref is not None:
        lane = lax.broadcasted_iota(jnp.int32, (batch, LANES), 1)
        rest = jnp.sum(squares, axis=1, keepdims=True)
        terms = jnp.zeros((batch, LANES), jnp.float32)
        for term in range(3):
            rounded = rest.astype(jnp.bfloat16).astype(jnp.float32)
            terms = jnp.where(lane == term, rounded, terms)
            rest = rest - rounded
        squares_ref[...] = terms.astype(squares_ref.dtype)


def multiply_kernel(relatives, count, with_squares, me_ref, *refs):
    piece_refs, refs = refs[:count], refs[count:]
    inverse_ref = squares_ref = None
    if with_squares:
        inverse_ref, refs = refs[0], refs[1:]
    w_refs, refs = refs[:SLABS], refs[SLABS:]
    scale_ref, undo_ref, *out_refs = refs[:-2]
    x_perm, product = refs[-2:]
    if with_squares:
        squares_ref = out_refs.pop()

    @pl.when(pl.program_id(0) == 0)
    def _():
        order_inputs(relatives, me_ref[0], piece_refs, x_perm, inverse_ref, squares_ref)

    slab = w_refs[0].shape[0]
    total = sum(
        jnp.dot(x_perm[:, q * slab : (q + 1) * slab], w_ref[...], preferred_element_type=jnp.float32)
        for q, w_ref in enumerate(w_refs)
    )
    product[...] = total * (scale_ref[...] * undo_ref[0:1, 0:1])
    rows = out_refs[0].shape[0]
    for relative, out_ref in enumerate(out_refs):
        first = 0 if len(out_refs) == 1 else pl.multiple_of((me_ref[1] ^ relative) * rows, rows)
        out_ref[...] = product[pl.ds(first, rows), :].astype(out_ref.dtype)


def multiply(gathered, w, scale, undo, steps, width, splits, name, inverse=None):
    relatives, pieces, me = gathered
    _, features, _ = w.shape
    first, count = steps
    batch = pieces[0].shape[1]
    more = [] if inverse is None else [inverse]
    out_specs = [pl.BlockSpec((batch // splits, width), lambda n: (0, n))] * splits
    out_shape = [jax.ShapeDtypeStruct((batch // splits, width * count), jnp.bfloat16)] * splits
    if more:
        out_specs = out_specs + [pl.BlockSpec((batch, LANES), lambda n: (0, 0))]
        out_shape = out_shape + [jax.ShapeDtypeStruct((batch, LANES), jnp.bfloat16)]
    return pl.pallas_call(
        functools.partial(multiply_kernel, relatives, len(pieces), inverse is not None),
        grid=(count,),
        in_specs=[pl.BlockSpec(memory_space=pltpu.SMEM)]
        + [pl.BlockSpec(p.shape, lambda n: (0, 0, 0)) for p in pieces]
        + [pl.BlockSpec(p.shape, lambda n: (0, 0)) for p in more]
        + [
            pl.BlockSpec((None, features // SLABS, width), lambda n, q=q: (n + first, q, 0))
            for q in range(SLABS)
        ]
        + [
            pl.BlockSpec((1, width), lambda n: (0, n + first)),
            pl.BlockSpec(undo.shape, lambda n: (0, 0)),
        ],
        out_specs=out_specs,
        out_shape=out_shape,
        scratch_shapes=[
            pltpu.VMEM((batch, features), jnp.bfloat16),
            pltpu.VMEM((batch, width), jnp.float32),
        ],
        compiler_params=pltpu.CompilerParams(vmem_limit_bytes=50 * MIB),
        cost_estimate=pl.CostEstimate(
            flops=4 * batch * features * width * count,
            bytes_accessed=2 * features * width * count,
            transcendentals=0,
        ),
        name=name,
    )(me, *pieces, *more, *([w] * SLABS), scale, undo)


def late_kernel(relatives, count, with_squares, chunk, me_ref, *refs):
    piece_refs, refs = refs[:count], refs[count:]
    inverse_ref = squares_ref = None
    if with_squares:
        inverse_ref, refs = refs[0], refs[1:]
    codes_ref, table_ref, terms_ref, w_ref, now_scale_ref, old_scale_ref, undo_ref, *out_refs = refs[:-6]
    x_perm, w_even, w_odd, old_total, now_total, squares = refs[-6:]
    if with_squares:
        squares_ref = squares
    features = x_perm.shape[1]
    width = w_ref.shape[1]
    chunks = features // chunk
    pairs = chunk // (2 * BLOCK)

    @pl.when(pl.program_id(0) == 0)
    def _():
        order_inputs(relatives, me_ref[0], piece_refs, x_perm, inverse_ref, squares_ref)

    def fill(c, into_ref):
        decode_rows(c * pairs, pairs, width, codes_ref, table_ref, terms_ref, into_ref, 0)

    def rows_of(c):
        return pl.ds(pl.multiple_of(c * chunk, chunk), chunk)

    def add(c, from_ref):
        now_total[...] += jnp.dot(x_perm[:, rows_of(c)], from_ref[...], preferred_element_type=jnp.float32)

    def add_old(c):
        old_total[...] += jnp.dot(
            x_perm[:, rows_of(c)], w_ref[rows_of(c), :], preferred_element_type=jnp.float32
        )

    now_total[...] = jnp.zeros_like(now_total)
    old_total[...] = jnp.zeros_like(old_total)
    w_odd[...] = jnp.zeros_like(w_odd)

    def pair(i, carry):
        fill(2 * i, w_even)
        add(jnp.maximum(2 * i - 1, 0), w_odd)
        add_old(2 * i)
        fill(2 * i + 1, w_odd)
        add(2 * i, w_even)
        add_old(2 * i + 1)
        return carry

    lax.fori_loop(0, chunks // 2, pair, 0)
    add(chunks - 1, w_odd)
    undo = undo_ref[0:1, 0:1]
    old_total[...] = old_total[...] * (old_scale_ref[...] * undo)
    now_total[...] = now_total[...] * (now_scale_ref[...] * undo)
    rows = out_refs[0].shape[1]
    for relative, out_ref in enumerate(out_refs):
        first = pl.multiple_of((me_ref[1] ^ relative) * rows, rows)
        at = pl.ds(pl.multiple_of(pl.program_id(0) * width, width), width) if with_squares else slice(None)
        out_ref[0, :, at] = old_total[pl.ds(first, rows), :].astype(out_ref.dtype)
        out_ref[1, :, at] = now_total[pl.ds(first, rows), :].astype(out_ref.dtype)
        if with_squares:
            last = out_ref.shape[2] - LANES
            out_ref[0, :, last:] = squares[pl.ds(first, rows), :].astype(out_ref.dtype)
            out_ref[1, :, last:] = jnp.zeros((rows, LANES), out_ref.dtype)


def late(gathered, codes, tables, w, scale, undo, now, old, count, width, splits, name, inverse=None):
    relatives, pieces, me = gathered
    _, features, _ = w.shape
    batch = pieces[0].shape[1]
    more = [] if inverse is None else [inverse]
    chunk = min(CHUNK, features // 2)
    rows = batch // splits
    columns = width * count + (LANES if more else 0)
    block = pl.BlockSpec((2, rows, width), lambda n: (0, 0, n))
    if more:
        block = pl.BlockSpec((2, rows, columns), lambda n: (0, 0, 0))
    out_specs = [block] * splits
    out_shape = [jax.ShapeDtypeStruct((2, rows, columns), jnp.bfloat16)] * splits
    return pl.pallas_call(
        functools.partial(late_kernel, relatives, len(pieces), inverse is not None, chunk),
        grid=(count,),
        in_specs=[pl.BlockSpec(memory_space=pltpu.SMEM)]
        + [pl.BlockSpec(p.shape, lambda n: (0, 0, 0)) for p in pieces]
        + [pl.BlockSpec(p.shape, lambda n: (0, 0)) for p in more]
        + [
            pl.BlockSpec((2, features // GROUP, width), lambda n: (0, 0, n + now)),
            pl.BlockSpec(tables[0].shape, lambda n: (0, 0, 0)),
            pl.BlockSpec(tables[1].shape, lambda n: (0, 0, 0)),
            pl.BlockSpec((None, features, width), lambda n: (n + old, 0, 0)),
            pl.BlockSpec((1, width), lambda n: (0, n + now)),
            pl.BlockSpec((1, width), lambda n: (0, n + old)),
            pl.BlockSpec(undo.shape, lambda n: (0, 0)),
        ],
        out_specs=out_specs,
        out_shape=out_shape,
        scratch_shapes=[
            pltpu.VMEM((batch, features), jnp.bfloat16),
            pltpu.VMEM((chunk, width), jnp.bfloat16),
            pltpu.VMEM((chunk, width), jnp.bfloat16),
            pltpu.VMEM((batch, width), jnp.float32),
            pltpu.VMEM((batch, width), jnp.float32),
            pltpu.VMEM((batch, LANES), jnp.float32),
        ],
        compiler_params=pltpu.CompilerParams(vmem_limit_bytes=50 * MIB),
        cost_estimate=pl.CostEstimate(
            flops=features * width * count * 1024,
            bytes_accessed=3 * features * width * count,
            transcendentals=0,
        ),
        name=name,
    )(me, *pieces, *more, codes, *tables, w, scale, scale, undo)


def exchange(x, move):
    inp, out = lax.axis_size("inp"), lax.axis_size("out")
    pairs = []
    for i in range(inp):
        for o in range(out):
            to_i, to_o = move(i, o)
            pairs.append((i * out + o, to_i * out + to_o))
    return lax.ppermute(x, ("inp", "out"), pairs)


def gather_out(x, cover):
    out = lax.axis_size("out")
    stacks, order = [x[None]], [0]
    for n in range(out.bit_length() - 1):
        bit = out >> (n + 1)
        sent = stacks[0] if n == 0 else jnp.concatenate(stacks)
        (arrived,) = cover(n, [exchange(sent, lambda i, o: (i, o ^ bit))])
        stacks.append(arrived)
        order = order + [r ^ bit for r in order]
    return stacks, order


def whole_rows(stacks, order):
    out = lax.axis_size("out")
    me = lax.axis_index("out").astype(jnp.int32)
    _, rows, width = stacks[0].shape
    if width % LANES:
        place = jnp.array([order.index(r) for r in range(out)], jnp.int32)
        stack = jnp.take(jnp.concatenate(stacks), place[me ^ jnp.arange(out, dtype=jnp.int32)], axis=0)
        stacks = [jnp.transpose(stack, (1, 0, 2)).reshape(1, rows, out * width)]
        order, me = [0], jnp.zeros_like(me)
    return tuple(order), stacks, jnp.stack([me, lax.axis_index("inp").astype(jnp.int32)])


def split_inp(partial, axis):
    inp = lax.axis_size("inp")
    me = lax.axis_index("inp")
    block = partial.shape[axis] // inp
    blocks = [
        lax.dynamic_slice_in_dim(partial, (me ^ d) * block, block, axis) for d in range(inp)
    ]
    return blocks[0], blocks[1:]


def send_inp(blocks):
    return [exchange(b, lambda i, o, d=d: (i ^ d, o)) for d, b in enumerate(blocks, start=1)]


def add_up(terms):
    total = terms[0].astype(jnp.float32)
    for term in terms[1:]:
        total = total + term.astype(jnp.float32)
    return total


def scatter_sum(partial, axis, cover=None):
    kept, leaving = split_inp(partial, axis)
    arrived = send_inp(leaving)
    if cover is not None:
        arrived = cover(arrived)
    return add_up([kept] + arrived)


def side_kernel(order, me_ref, *refs):
    out_ref = refs[-1]
    listed = [(n, ref) for ref in refs[:-1] for n in range(ref.shape[0])]
    for relative, (n, ref) in zip(order, listed):
        width = ref.shape[2]
        at = pl.ds(pl.multiple_of((me_ref[0] ^ relative) * width, LANES), width)
        out_ref[:, at] = ref[n]


def side_by_side(stacks, order):
    inp = lax.axis_size("inp")
    me = lax.axis_index("inp").astype(jnp.int32)
    _, rows, width = stacks[0].shape
    if width % LANES:
        place = jnp.array([order.index(r) for r in range(inp)], jnp.int32)
        stack = jnp.take(jnp.concatenate(stacks), place[me ^ jnp.arange(inp, dtype=jnp.int32)], axis=0)
        return jnp.transpose(stack, (1, 0, 2)).reshape(rows, inp * width)
    return pl.pallas_call(
        functools.partial(side_kernel, tuple(order)),
        in_specs=[pl.BlockSpec(memory_space=pltpu.SMEM)]
        + [pl.BlockSpec(memory_space=pltpu.VMEM)] * len(stacks),
        out_shape=jax.ShapeDtypeStruct((rows, inp * width), stacks[0].dtype),
        name="side_by_side",
    )(me[None], *stacks)


def finish_kernel(inp, spans, model, *refs):
    out_ref, refs = refs[-1], refs[:-1]
    columns = spans[0][1]
    terms = sum(ref[0, :, columns:].astype(jnp.float32) for ref in refs[:inp])
    factor = lax.rsqrt(jnp.sum(terms, axis=1, keepdims=True) / model + epsilon)
    for n, (starts, columns) in enumerate(spans):
        parts = refs[n * inp : (n + 1) * inp]
        for half, start in enumerate(starts):
            at = (half, slice(None), slice(columns)) if len(parts[0].shape) == 3 else slice(None)
            total = sum(part[at].astype(jnp.float32) for part in parts)
            out_ref[:, start : start + columns] = (total * factor).astype(jnp.bfloat16)


def finish(blocks, spans, rows, outputs, model):
    operands = [piece for block in blocks for piece in block]
    return pl.pallas_call(
        functools.partial(finish_kernel, len(blocks[0]), tuple(spans), model),
        in_specs=[pl.BlockSpec(memory_space=pltpu.VMEM)] * len(operands),
        out_shape=jax.ShapeDtypeStruct((rows, outputs), jnp.bfloat16),
        compiler_params=pltpu.CompilerParams(vmem_limit_bytes=16 * MIB),
        name="finish",
    )(*operands)


class Ahead:
    def __init__(self, codes, tables, scale, name):
        *self.tables, self.undo = tables
        self.codes, self.name = codes, name
        self.scale = scale[None, :]
        self.width = math.gcd(codes.shape[2], 256)
        self.steps = codes.shape[2] // self.width
        self.done = 0
        self.limit = self.steps
        self.buffer = None

    def run(self, count):
        count = min(count, self.limit - self.done)
        if count > 0:
            self.buffer = decode(
                self.codes, self.tables, (self.done, count), self.width, self.buffer, self.name
            )
            self.done += count

    def after(self, arrays):
        if self.buffer is None:
            self.codes, *arrays = lax.optimization_barrier((self.codes, *arrays))
        else:
            self.buffer, *arrays = lax.optimization_barrier((self.buffer, *arrays))
        return arrays

    def beside(self, count, arrays):
        self.run(count)
        return self.after(arrays)


def per_device(
    attention, residual, wo_codes, wo_books, wo_scale, norm_gain, gate_codes, gate_books, gate_scale
):
    inp = lax.axis_size("inp")
    out = lax.axis_size("out")
    inp_at = lax.axis_index("inp")
    out_at = lax.axis_index("out")
    model = norm_gain.shape[0]
    wo_tables, gate_tables = make_tables(wo_books, gate_books)
    wo = Ahead(wo_codes, wo_tables, wo_scale, "decode_wo")
    gate = Ahead(gate_codes, gate_tables, gate_scale, "decode_gate")
    share = gate.steps / 26
    gate.limit = (gate.steps + 1) // 2

    def early(n, arrays):
        if n < 2:
            return wo.beside(wo.steps * 3 // 8, arrays)
        wo.run(wo.steps)
        gate.codes, wo.buffer = lax.optimization_barrier((gate.codes, wo.buffer))
        return gate.beside(int(COVER[0] * share), arrays)

    gathered = whole_rows(*gather_out(attention, early))
    (partial,) = multiply(
        gathered, wo.buffer, wo.scale, wo.undo, (0, wo.steps), wo.width, 1, "multiply_wo"
    )
    kept, leaving = split_inp(partial, 1)
    leaving = gate.after(leaving)
    arrived = gate.beside(int(COVER[1] * share), send_inp(leaving))
    piece = kept.shape[1]
    own = lax.dynamic_slice_in_dim(residual, inp_at * piece, piece, 1)
    hidden = own.astype(jnp.float32) + add_up([kept] + arrived)
    gain = lax.dynamic_slice_in_dim(norm_gain, (out_at * inp + inp_at) * piece, piece, 0)
    gained = (hidden * gain[None, :]).astype(jnp.bfloat16)
    rounded = hidden.astype(jnp.bfloat16)

    per_block = out // inp
    gained, rounded = gate.after([gained, rounded])
    (moved,) = gate.beside(
        int(COVER[2] * share),
        [exchange(gained, lambda q, o: (o // per_block, (o % per_block) * inp + q))],
    )
    stream_stacks, stream_order = [rounded[None]], [0]

    def beside_rounds(n, arrays):
        bit = 1 << n
        count = int(COVER[min(3 + n, 4)] * share) if 2 << n < out else gate.steps
        if bit >= inp:
            return gate.beside(count, arrays)
        sent = jnp.concatenate(stream_stacks) if n else stream_stacks[0]
        more = exchange(sent, lambda i, o: (i ^ bit, o))
        arrived, more = gate.beside(count, arrays + [more])
        stream_order.extend([r ^ bit for r in stream_order])
        stream_stacks.append(more)
        return [arrived]

    relatives, stacks, me = whole_rows(*gather_out(moved, beside_rounds))
    stream = side_by_side(stream_stacks, stream_order)

    block = model // inp
    inverse = 1.0 / lax.dynamic_slice_in_dim(norm_gain, inp_at * block, block, 0)[None, :]
    pairs = gate.steps - gate.done
    single = gate.done - pairs
    jobs = []
    start = single
    for count in (pairs - pairs * 4 // 13, pairs * 4 // 13):
        jobs.append((start, count))
        start += count
    if single:
        jobs.append((0, single))
    blocks = []
    waiting = None
    for first, count in jobs:
        given = (relatives, stacks, me)
        if first < single:
            parts = multiply(
                given, gate.buffer, gate.scale, gate.undo, (first, count), gate.width, inp, "multiply_gate"
            )
        else:
            parts = late(
                given,
                gate.codes,
                gate.tables,
                gate.buffer,
                gate.scale,
                gate.undo,
                gate.done + first - single,
                first,
                count,
                gate.width,
                inp,
                "late_gate",
                None if blocks or waiting else inverse,
            )
        parts = list(parts)
        if waiting is not None:
            kept, arrived = waiting
            arrived, parts = lax.optimization_barrier((arrived, parts))
            blocks.append([kept] + arrived)
        kept, *leaving = parts
        leaving, stacks = lax.optimization_barrier((leaving, stacks))
        waiting = (kept, send_inp(leaving))
    kept, arrived = waiting
    blocks.append([kept] + arrived)
    width = gate.width
    spans = []
    for first, count in jobs:
        starts = (first * width,)
        if first >= single:
            starts += ((gate.done + first - single) * width,)
        spans.append((starts, count * width))
    gate_out = finish(blocks, spans, attention.shape[0] // inp, gate.steps * width, model)
    return (stream, gate_out)


def solution(mesh):
    placed = (
        P(None, ("inp", "out")),
        P(None, "out"),
        P(None, "inp", "out"),
        P(),
        P("out"),
        P(),
        P(None, "inp", "out"),
        P(),
        P("out"),
    )
    return jax.shard_map(
        per_device,
        mesh=mesh,
        in_specs=placed,
        out_specs=(P(None, "out"), P("inp", "out")),
        check_vma=False,
    )
```

```python
import functools
import math

import jax
import jax.numpy as jnp
from jax import lax
from jax.experimental import pallas as pl
from jax.experimental.pallas import tpu as pltpu
from jax.sharding import PartitionSpec as P


epsilon = 1e-05
LANES = 128
GROUP = 8
ROWS = 16
BLOCK = ROWS * GROUP
MIB = 1024 * 1024
UNROLL = 16
PART = 256
CHUNK = 1024
SLABS = 4
COVER = (0, 2, 2, 2, 2)

take_lanes = lax.GatherDimensionNumbers(
    offset_dims=(),
    collapsed_slice_dims=(1,),
    start_index_map=(1,),
    operand_batching_dims=(0,),
    start_indices_batching_dims=(0,),
)


take_rows = lax.GatherDimensionNumbers(
    offset_dims=(),
    collapsed_slice_dims=(0,),
    start_index_map=(0,),
    operand_batching_dims=(1,),
    start_indices_batching_dims=(1,),
)

BY_LANE = 5
PAIR = 2 * ROWS


def lookup(table, index, dims=take_lanes):
    return lax.gather(
        table,
        index[..., None],
        dims,
        slice_sizes=(1, 1),
        mode=lax.GatherScatterMode.PROMISE_IN_BOUNDS,
    )


def tables_kernel(*refs):
    count = len(refs) // 4
    for books_ref, lanes_ref, rows_ref, undo_ref in zip(*(refs[n * count : (n + 1) * count] for n in range(4))):
        books, group, entries = books_ref.shape
        values = books_ref[...].astype(jnp.float32)
        top = jnp.max(jnp.abs(values), axis=(0, 1, 2), keepdims=True)[0]
        top = jnp.maximum(top, 2.0**-60)
        factor = jnp.ones_like(top)
        for step in (64, 32, 16, 8, 4, 2, 1):
            more = factor * 2.0**step
            factor = jnp.where(top * more <= 224.0, more, factor)
        undo_ref[...] = jnp.broadcast_to(1.0 / factor, undo_ref.shape)
        row = lax.broadcasted_iota(jnp.int32, (group, LANES), 0)
        for book in range(books):
            scaled = values[book] * factor
            for half in range(entries // LANES):
                at = slice(half * LANES, (half + 1) * LANES)
                for k in range(BY_LANE):
                    lanes_ref[(book * 2 + half) * group + k] = jnp.broadcast_to(
                        scaled[k : k + 1, at], (ROWS, LANES)
                    ).astype(jnp.bfloat16)
            for k in range(BY_LANE, group):
                pick = jnp.where(row == k, 1.0, 0.0).astype(jnp.bfloat16)
                column = lax.dot_general(
                    scaled.astype(jnp.bfloat16), pick, (((0,), (0,)), ((), ())), preferred_element_type=jnp.float32
                )
                first = column.astype(jnp.float8_e4m3fn)
                second = ((column - first.astype(jnp.float32)) * 16.0).astype(jnp.float8_e4m3fn)
                parts = entries // PAIR
                for term, terms in enumerate((first, second)):
                    base = (((k - BY_LANE) * 2 + book) * 2 + term) * parts
                    for part in range(parts):
                        rows_ref[base + part] = terms[part * PAIR : (part + 1) * PAIR]


def make_tables(*all_books):
    turned = [jnp.swapaxes(books, 1, 2) for books in all_books]
    count = len(turned)
    lanes, rows, undo = [], [], []
    for books, group, entries in (t.shape for t in turned):
        lanes.append(jax.ShapeDtypeStruct((books * (entries // LANES) * group, ROWS, LANES), jnp.bfloat16))
        parts = (group - BY_LANE) * books * 2 * (entries // PAIR)
        rows.append(jax.ShapeDtypeStruct((parts, PAIR, LANES), jnp.float8_e4m3fn))
        undo.append(jax.ShapeDtypeStruct((1, LANES), jnp.float32))
    made = pl.pallas_call(tables_kernel, out_shape=lanes + rows + undo, name="make_tables")(*turned)
    return [(made[n], made[count + n], made[2 * count + n]) for n in range(count)]


def decode_block(codes, table_ref, terms):
    rows = [[], []]
    picked = [[], []]
    for half in range(2):
        for book, code in enumerate(codes):
            narrow = code[half * ROWS : (half + 1) * ROWS].astype(jnp.int16)
            low = narrow < LANES
            index = narrow & (LANES - 1)
            first = [lookup(table_ref[(book * 2) * GROUP + k], index) for k in range(BY_LANE)]
            second = [lookup(table_ref[(book * 2 + 1) * GROUP + k], index) for k in range(BY_LANE)]
            picked[book] = [jnp.where(low, a, b) for a, b in zip(first, second)]
        rows[half] = [a + b for a, b in zip(*picked)]
    if BY_LANE == GROUP:
        return rows
    index, bits = [], []
    for code in codes:
        low = (code & (LANES - 1)).astype(jnp.int8)
        high = (code >> 7).astype(jnp.int8)
        index.append(low & (PAIR - 1))
        bits.append([(low & 32) != 0, (low & 64) != 0, high != 0])
    parts = 8
    for k in range(GROUP - BY_LANE):
        sums = []
        for term in range(2):
            total = None
            for book in range(2):
                base = ((k * 2 + book) * 2 + term) * parts
                level = [lookup(terms[base + t], index[book], take_rows) for t in range(parts)]
                for bit in bits[book]:
                    level = [jnp.where(bit, level[n + 1], level[n]) for n in range(0, len(level), 2)]
                value = level[0].astype(jnp.bfloat16)
                total = value if total is None else total + value
            sums.append(total)
        value = sums[0] + sums[1] * jnp.bfloat16(0.0625)
        for half in range(2):
            rows[half].append(value[half * ROWS : (half + 1) * ROWS])
    return rows


def decode_rows(first_pair, pairs, width, codes_ref, table_ref, terms_ref, w_ref, first_row):
    terms = [terms_ref[n] for n in range(terms_ref.shape[0])]
    for b in range(pairs):
        groups = pl.ds(pl.multiple_of((first_pair + b) * PAIR, PAIR), PAIR)
        for j in range(0, width, LANES):
            codes = [codes_ref[book, groups, j : j + LANES] for book in range(2)]
            for half, values in enumerate(decode_block(codes, table_ref, terms)):
                for k, rows in enumerate(values):
                    at = pl.multiple_of(first_row + (2 * b + half) * BLOCK, BLOCK) + k * ROWS
                    w_ref[pl.ds(at, ROWS), j : j + LANES] = rows


def decode_kernel(unroll, codes_ref, table_ref, terms_ref, *rest):
    w_ref = rest[-1]
    pairs = codes_ref.shape[1] // PAIR

    def some(i, carry):
        first = i * unroll
        row = first * 2 * BLOCK
        decode_rows(first, unroll, w_ref.shape[1], codes_ref, table_ref, terms_ref, w_ref, row)
        return carry

    lax.fori_loop(0, pairs // unroll, some, 0)


def decode(codes, tables, steps, width, into=None, name="decode"):
    _, groups, outputs = codes.shape
    first, count = steps
    part = math.gcd(width, PART if count > 2 else LANES)
    cuts = width // part
    operands = [codes, *tables]
    in_specs = [
        pl.BlockSpec((2, groups, part), lambda n: (0, 0, n + first * cuts)),
        pl.BlockSpec(tables[0].shape, lambda n: (0, 0, 0)),
        pl.BlockSpec(tables[1].shape, lambda n: (0, 0, 0)),
    ]
    aliases = {}
    if into is not None:
        operands.append(into)
        in_specs.append(pl.BlockSpec(memory_space=pl.ANY))
        aliases = {3: 0}
    return pl.pallas_call(
        functools.partial(decode_kernel, min(UNROLL * 128 // part, groups // PAIR)),
        grid=(count * cuts,),
        in_specs=in_specs,
        out_specs=pl.BlockSpec((None, groups * GROUP, part), lambda n: (first + n // cuts, 0, n % cuts)),
        out_shape=jax.ShapeDtypeStruct((outputs // width, groups * GROUP, width), jnp.bfloat16),
        input_output_aliases=aliases,
        compiler_params=pltpu.CompilerParams(vmem_limit_bytes=58 * MIB),
        cost_estimate=pl.CostEstimate(
            flops=groups * width * count * 8192,
            bytes_accessed=24 * groups * width * count,
            transcendentals=0,
        ),
        name=name,
    )(*operands)


def order_inputs(relatives, me, piece_refs, x_perm, inverse_ref=None, squares_ref=None):
    row = lax.broadcasted_iota(jnp.int32, (LANES, LANES), 0)
    col = lax.broadcasted_iota(jnp.int32, (LANES, LANES), 1)
    source = (col % ROWS) * GROUP + col // ROWS
    swap = jnp.where(row == source, 1.0, 0.0).astype(jnp.bfloat16)
    batch = x_perm.shape[0]
    squares = jnp.zeros((batch, LANES), jnp.float32)
    listed = [(n, ref) for ref in piece_refs for n in range(ref.shape[0])]
    for relative, (n, ref) in zip(relatives, listed):
        piece = ref.shape[2]
        for c in range(0, piece, LANES):
            columns = pl.ds(pl.multiple_of((me ^ relative) * piece + c, LANES), LANES)
            values = ref[n, :, c : c + LANES]
            x_perm[:, columns] = jnp.dot(values, swap, preferred_element_type=jnp.float32).astype(
                jnp.bfloat16
            )
            if squares_ref is not None:
                plain = values.astype(jnp.float32) * inverse_ref[:, columns]
                squares = squares + plain * plain
    if squares_ref is not None:
        lane = lax.broadcasted_iota(jnp.int32, (batch, LANES), 1)
        rest = jnp.sum(squares, axis=1, keepdims=True)
        terms = jnp.zeros((batch, LANES), jnp.float32)
        for term in range(3):
            rounded = rest.astype(jnp.bfloat16).astype(jnp.float32)
            terms = jnp.where(lane == term, rounded, terms)
            rest = rest - rounded
        squares_ref[...] = terms.astype(squares_ref.dtype)


def multiply_kernel(relatives, count, with_squares, me_ref, *refs):
    piece_refs, refs = refs[:count], refs[count:]
    inverse_ref = squares_ref = None
    if with_squares:
        inverse_ref, refs = refs[0], refs[1:]
    w_refs, refs = refs[:SLABS], refs[SLABS:]
    scale_ref, undo_ref, *out_refs = refs[:-2]
    x_perm, product = refs[-2:]
    if with_squares:
        squares_ref = out_refs.pop()

    @pl.when(pl.program_id(0) == 0)
    def _():
        order_inputs(relatives, me_ref[0], piece_refs, x_perm, inverse_ref, squares_ref)

    slab = w_refs[0].shape[0]
    total = sum(
        jnp.dot(x_perm[:, q * slab : (q + 1) * slab], w_ref[...], preferred_element_type=jnp.float32)
        for q, w_ref in enumerate(w_refs)
    )
    product[...] = total * (scale_ref[...] * undo_ref[0:1, 0:1])
    rows = out_refs[0].shape[0]
    for relative, out_ref in enumerate(out_refs):
        first = 0 if len(out_refs) == 1 else pl.multiple_of((me_ref[1] ^ relative) * rows, rows)
        out_ref[...] = product[pl.ds(first, rows), :].astype(out_ref.dtype)


def multiply(gathered, w, scale, undo, steps, width, splits, name, inverse=None):
    relatives, pieces, me = gathered
    _, features, _ = w.shape
    first, count = steps
    batch = pieces[0].shape[1]
    more = [] if inverse is None else [inverse]
    out_specs = [pl.BlockSpec((batch // splits, width), lambda n: (0, n))] * splits
    out_shape = [jax.ShapeDtypeStruct((batch // splits, width * count), jnp.bfloat16)] * splits
    if more:
        out_specs = out_specs + [pl.BlockSpec((batch, LANES), lambda n: (0, 0))]
        out_shape = out_shape + [jax.ShapeDtypeStruct((batch, LANES), jnp.bfloat16)]
    return pl.pallas_call(
        functools.partial(multiply_kernel, relatives, len(pieces), inverse is not None),
        grid=(count,),
        in_specs=[pl.BlockSpec(memory_space=pltpu.SMEM)]
        + [pl.BlockSpec(p.shape, lambda n: (0, 0, 0)) for p in pieces]
        + [pl.BlockSpec(p.shape, lambda n: (0, 0)) for p in more]
        + [
            pl.BlockSpec((None, features // SLABS, width), lambda n, q=q: (n + first, q, 0))
            for q in range(SLABS)
        ]
        + [
            pl.BlockSpec((1, width), lambda n: (0, n + first)),
            pl.BlockSpec(undo.shape, lambda n: (0, 0)),
        ],
        out_specs=out_specs,
        out_shape=out_shape,
        scratch_shapes=[
            pltpu.VMEM((batch, features), jnp.bfloat16),
            pltpu.VMEM((batch, width), jnp.float32),
        ],
        compiler_params=pltpu.CompilerParams(vmem_limit_bytes=50 * MIB),
        cost_estimate=pl.CostEstimate(
            flops=4 * batch * features * width * count,
            bytes_accessed=2 * features * width * count,
            transcendentals=0,
        ),
        name=name,
    )(me, *pieces, *more, *([w] * SLABS), scale, undo)


def late_kernel(relatives, count, with_squares, chunk, me_ref, *refs):
    piece_refs, refs = refs[:count], refs[count:]
    inverse_ref = squares_ref = None
    if with_squares:
        inverse_ref, refs = refs[0], refs[1:]
    codes_ref, table_ref, terms_ref, w_ref, now_scale_ref, old_scale_ref, undo_ref, *out_refs = refs[:-6]
    x_perm, w_even, w_odd, old_total, now_total, squares = refs[-6:]
    if with_squares:
        squares_ref = squares
    features = x_perm.shape[1]
    width = w_ref.shape[1]
    chunks = features // chunk
    pairs = chunk // (2 * BLOCK)

    @pl.when(pl.program_id(0) == 0)
    def _():
        order_inputs(relatives, me_ref[0], piece_refs, x_perm, inverse_ref, squares_ref)

    def fill(c, into_ref):
        decode_rows(c * pairs, pairs, width, codes_ref, table_ref, terms_ref, into_ref, 0)

    def rows_of(c):
        return pl.ds(pl.multiple_of(c * chunk, chunk), chunk)

    def add(c, from_ref):
        now_total[...] += jnp.dot(x_perm[:, rows_of(c)], from_ref[...], preferred_element_type=jnp.float32)

    def add_old(c):
        old_total[...] += jnp.dot(
            x_perm[:, rows_of(c)], w_ref[rows_of(c), :], preferred_element_type=jnp.float32
        )

    now_total[...] = jnp.zeros_like(now_total)
    old_total[...] = jnp.zeros_like(old_total)
    w_odd[...] = jnp.zeros_like(w_odd)

    def pair(i, carry):
        fill(2 * i, w_even)
        add(jnp.maximum(2 * i - 1, 0), w_odd)
        add_old(2 * i)
        fill(2 * i + 1, w_odd)
        add(2 * i, w_even)
        add_old(2 * i + 1)
        return carry

    lax.fori_loop(0, chunks // 2, pair, 0)
    add(chunks - 1, w_odd)
    undo = undo_ref[0:1, 0:1]
    old_total[...] = old_total[...] * (old_scale_ref[...] * undo)
    now_total[...] = now_total[...] * (now_scale_ref[...] * undo)
    rows = out_refs[0].shape[1]
    for relative, out_ref in enumerate(out_refs):
        first = pl.multiple_of((me_ref[1] ^ relative) * rows, rows)
        at = pl.ds(pl.multiple_of(pl.program_id(0) * width, width), width) if with_squares else slice(None)
        out_ref[0, :, at] = old_total[pl.ds(first, rows), :].astype(out_ref.dtype)
        out_ref[1, :, at] = now_total[pl.ds(first, rows), :].astype(out_ref.dtype)
        if with_squares:
            last = out_ref.shape[2] - LANES
            out_ref[0, :, last:] = squares[pl.ds(first, rows), :].astype(out_ref.dtype)
            out_ref[1, :, last:] = jnp.zeros((rows, LANES), out_ref.dtype)


def late(gathered, codes, tables, w, scale, undo, now, old, count, width, splits, name, inverse=None):
    relatives, pieces, me = gathered
    _, features, _ = w.shape
    batch = pieces[0].shape[1]
    more = [] if inverse is None else [inverse]
    chunk = min(CHUNK, features // 2)
    rows = batch // splits
    columns = width * count + (LANES if more else 0)
    block = pl.BlockSpec((2, rows, width), lambda n: (0, 0, n))
    if more:
        block = pl.BlockSpec((2, rows, columns), lambda n: (0, 0, 0))
    out_specs = [block] * splits
    out_shape = [jax.ShapeDtypeStruct((2, rows, columns), jnp.bfloat16)] * splits
    return pl.pallas_call(
        functools.partial(late_kernel, relatives, len(pieces), inverse is not None, chunk),
        grid=(count,),
        in_specs=[pl.BlockSpec(memory_space=pltpu.SMEM)]
        + [pl.BlockSpec(p.shape, lambda n: (0, 0, 0)) for p in pieces]
        + [pl.BlockSpec(p.shape, lambda n: (0, 0)) for p in more]
        + [
            pl.BlockSpec((2, features // GROUP, width), lambda n: (0, 0, n + now)),
            pl.BlockSpec(tables[0].shape, lambda n: (0, 0, 0)),
            pl.BlockSpec(tables[1].shape, lambda n: (0, 0, 0)),
            pl.BlockSpec((None, features, width), lambda n: (n + old, 0, 0)),
            pl.BlockSpec((1, width), lambda n: (0, n + now)),
            pl.BlockSpec((1, width), lambda n: (0, n + old)),
            pl.BlockSpec(undo.shape, lambda n: (0, 0)),
        ],
        out_specs=out_specs,
        out_shape=out_shape,
        scratch_shapes=[
            pltpu.VMEM((batch, features), jnp.bfloat16),
            pltpu.VMEM((chunk, width), jnp.bfloat16),
            pltpu.VMEM((chunk, width), jnp.bfloat16),
            pltpu.VMEM((batch, width), jnp.float32),
            pltpu.VMEM((batch, width), jnp.float32),
            pltpu.VMEM((batch, LANES), jnp.float32),
        ],
        compiler_params=pltpu.CompilerParams(vmem_limit_bytes=50 * MIB),
        cost_estimate=pl.CostEstimate(
            flops=features * width * count * 1024,
            bytes_accessed=3 * features * width * count,
            transcendentals=0,
        ),
        name=name,
    )(me, *pieces, *more, codes, *tables, w, scale, scale, undo)


def exchange(x, move):
    inp, out = lax.axis_size("inp"), lax.axis_size("out")
    pairs = []
    for i in range(inp):
        for o in range(out):
            to_i, to_o = move(i, o)
            pairs.append((i * out + o, to_i * out + to_o))
    return lax.ppermute(x, ("inp", "out"), pairs)


def gather_out(x, cover):
    out = lax.axis_size("out")
    stacks, order = [x[None]], [0]
    for n in range(out.bit_length() - 1):
        bit = out >> (n + 1)
        sent = stacks[0] if n == 0 else jnp.concatenate(stacks)
        (arrived,) = cover(n, [exchange(sent, lambda i, o: (i, o ^ bit))])
        stacks.append(arrived)
        order = order + [r ^ bit for r in order]
    return stacks, order


def whole_rows(stacks, order):
    out = lax.axis_size("out")
    me = lax.axis_index("out").astype(jnp.int32)
    _, rows, width = stacks[0].shape
    if width % LANES:
        place = jnp.array([order.index(r) for r in range(out)], jnp.int32)
        stack = jnp.take(jnp.concatenate(stacks), place[me ^ jnp.arange(out, dtype=jnp.int32)], axis=0)
        stacks = [jnp.transpose(stack, (1, 0, 2)).reshape(1, rows, out * width)]
        order, me = [0], jnp.zeros_like(me)
    return tuple(order), stacks, jnp.stack([me, lax.axis_index("inp").astype(jnp.int32)])


def split_inp(partial, axis):
    inp = lax.axis_size("inp")
    me = lax.axis_index("inp")
    block = partial.shape[axis] // inp
    blocks = [
        lax.dynamic_slice_in_dim(partial, (me ^ d) * block, block, axis) for d in range(inp)
    ]
    return blocks[0], blocks[1:]


def send_inp(blocks):
    return [exchange(b, lambda i, o, d=d: (i ^ d, o)) for d, b in enumerate(blocks, start=1)]


def add_up(terms):
    total = terms[0].astype(jnp.float32)
    for term in terms[1:]:
        total = total + term.astype(jnp.float32)
    return total


def scatter_sum(partial, axis, cover=None):
    kept, leaving = split_inp(partial, axis)
    arrived = send_inp(leaving)
    if cover is not None:
        arrived = cover(arrived)
    return add_up([kept] + arrived)


def side_kernel(order, me_ref, *refs):
    out_ref = refs[-1]
    listed = [(n, ref) for ref in refs[:-1] for n in range(ref.shape[0])]
    for relative, (n, ref) in zip(order, listed):
        width = ref.shape[2]
        at = pl.ds(pl.multiple_of((me_ref[0] ^ relative) * width, LANES), width)
        out_ref[:, at] = ref[n]


def side_by_side(stacks, order):
    inp = lax.axis_size("inp")
    me = lax.axis_index("inp").astype(jnp.int32)
    _, rows, width = stacks[0].shape
    if width % LANES:
        place = jnp.array([order.index(r) for r in range(inp)], jnp.int32)
        stack = jnp.take(jnp.concatenate(stacks), place[me ^ jnp.arange(inp, dtype=jnp.int32)], axis=0)
        return jnp.transpose(stack, (1, 0, 2)).reshape(rows, inp * width)
    return pl.pallas_call(
        functools.partial(side_kernel, tuple(order)),
        in_specs=[pl.BlockSpec(memory_space=pltpu.SMEM)]
        + [pl.BlockSpec(memory_space=pltpu.VMEM)] * len(stacks),
        out_shape=jax.ShapeDtypeStruct((rows, inp * width), stacks[0].dtype),
        name="side_by_side",
    )(me[None], *stacks)


def finish_kernel(inp, spans, model, *refs):
    out_ref, refs = refs[-1], refs[:-1]
    columns = spans[0][1]
    terms = sum(ref[0, :, columns:].astype(jnp.float32) for ref in refs[:inp])
    factor = lax.rsqrt(jnp.sum(terms, axis=1, keepdims=True) / model + epsilon)
    for n, (starts, columns) in enumerate(spans):
        parts = refs[n * inp : (n + 1) * inp]
        for half, start in enumerate(starts):
            at = (half, slice(None), slice(columns)) if len(parts[0].shape) == 3 else slice(None)
            total = sum(part[at].astype(jnp.float32) for part in parts)
            out_ref[:, start : start + columns] = (total * factor).astype(jnp.bfloat16)


def finish(blocks, spans, rows, outputs, model):
    operands = [piece for block in blocks for piece in block]
    return pl.pallas_call(
        functools.partial(finish_kernel, len(blocks[0]), tuple(spans), model),
        in_specs=[pl.BlockSpec(memory_space=pltpu.VMEM)] * len(operands),
        out_shape=jax.ShapeDtypeStruct((rows, outputs), jnp.bfloat16),
        compiler_params=pltpu.CompilerParams(vmem_limit_bytes=16 * MIB),
        name="finish",
    )(*operands)


class Ahead:
    def __init__(self, codes, tables, scale, name):
        *self.tables, self.undo = tables
        self.codes, self.name = codes, name
        self.scale = scale[None, :]
        self.width = math.gcd(codes.shape[2], 256)
        self.steps = codes.shape[2] // self.width
        self.done = 0
        self.limit = self.steps
        self.buffer = None

    def run(self, count):
        count = min(count, self.limit - self.done)
        if count > 0:
            self.buffer = decode(
                self.codes, self.tables, (self.done, count), self.width, self.buffer, self.name
            )
            self.done += count

    def after(self, arrays):
        if self.buffer is None:
            self.codes, *arrays = lax.optimization_barrier((self.codes, *arrays))
        else:
            self.buffer, *arrays = lax.optimization_barrier((self.buffer, *arrays))
        return arrays

    def beside(self, count, arrays):
        self.run(count)
        return self.after(arrays)


def per_device(
    attention, residual, wo_codes, wo_books, wo_scale, norm_gain, gate_codes, gate_books, gate_scale
):
    inp = lax.axis_size("inp")
    out = lax.axis_size("out")
    inp_at = lax.axis_index("inp")
    out_at = lax.axis_index("out")
    model = norm_gain.shape[0]
    wo_tables, gate_tables = make_tables(wo_books, gate_books)
    wo = Ahead(wo_codes, wo_tables, wo_scale, "decode_wo")
    gate = Ahead(gate_codes, gate_tables, gate_scale, "decode_gate")
    share = gate.steps / 26
    gate.limit = (gate.steps + 1) // 2

    def early(n, arrays):
        if n < 2:
            return wo.beside(wo.steps * 2 // 8, arrays)
        wo.run(wo.steps)
        gate.codes, wo.buffer = lax.optimization_barrier((gate.codes, wo.buffer))
        return gate.beside(int(COVER[0] * share), arrays)

    gathered = whole_rows(*gather_out(attention, early))
    (partial,) = multiply(
        gathered, wo.buffer, wo.scale, wo.undo, (0, wo.steps), wo.width, 1, "multiply_wo"
    )
    kept, leaving = split_inp(partial, 1)
    leaving = gate.after(leaving)
    arrived = gate.beside(int(COVER[1] * share), send_inp(leaving))
    piece = kept.shape[1]
    own = lax.dynamic_slice_in_dim(residual, inp_at * piece, piece, 1)
    hidden = own.astype(jnp.float32) + add_up([kept] + arrived)
    gain = lax.dynamic_slice_in_dim(norm_gain, (out_at * inp + inp_at) * piece, piece, 0)
    gained = (hidden * gain[None, :]).astype(jnp.bfloat16)
    rounded = hidden.astype(jnp.bfloat16)

    per_block = out // inp
    gained, rounded = gate.after([gained, rounded])
    (moved,) = gate.beside(
        int(COVER[2] * share),
        [exchange(gained, lambda q, o: (o // per_block, (o % per_block) * inp + q))],
    )
    stream_stacks, stream_order = [rounded[None]], [0]

    def beside_rounds(n, arrays):
        bit = 1 << n
        count = int(COVER[min(3 + n, 4)] * share) if 2 << n < out else gate.steps
        if bit >= inp:
            return gate.beside(count, arrays)
        sent = jnp.concatenate(stream_stacks) if n else stream_stacks[0]
        more = exchange(sent, lambda i, o: (i ^ bit, o))
        arrived, more = gate.beside(count, arrays + [more])
        stream_order.extend([r ^ bit for r in stream_order])
        stream_stacks.append(more)
        return [arrived]

    relatives, stacks, me = whole_rows(*gather_out(moved, beside_rounds))
    stream = side_by_side(stream_stacks, stream_order)

    block = model // inp
    inverse = 1.0 / lax.dynamic_slice_in_dim(norm_gain, inp_at * block, block, 0)[None, :]
    pairs = gate.steps - gate.done
    single = gate.done - pairs
    jobs = []
    start = single
    for count in (pairs - pairs * 4 // 13, pairs * 4 // 13):
        jobs.append((start, count))
        start += count
    if single:
        jobs.append((0, single))
    blocks = []
    waiting = None
    for first, count in jobs:
        given = (relatives, stacks, me)
        if first < single:
            parts = multiply(
                given, gate.buffer, gate.scale, gate.undo, (first, count), gate.width, inp, "multiply_gate"
            )
        else:
            parts = late(
                given,
                gate.codes,
                gate.tables,
                gate.buffer,
                gate.scale,
                gate.undo,
                gate.done + first - single,
                first,
                count,
                gate.width,
                inp,
                "late_gate",
                None if blocks or waiting else inverse,
            )
        parts = list(parts)
        if waiting is not None:
            kept, arrived = waiting
            arrived, parts = lax.optimization_barrier((arrived, parts))
            blocks.append([kept] + arrived)
        kept, *leaving = parts
        leaving, stacks = lax.optimization_barrier((leaving, stacks))
        waiting = (kept, send_inp(leaving))
    kept, arrived = waiting
    blocks.append([kept] + arrived)
    width = gate.width
    spans = []
    for first, count in jobs:
        starts = (first * width,)
        if first >= single:
            starts += ((gate.done + first - single) * width,)
        spans.append((starts, count * width))
    gate_out = finish(blocks, spans, attention.shape[0] // inp, gate.steps * width, model)
    return (stream, gate_out)


def solution(mesh):
    placed = (
        P(None, ("inp", "out")),
        P(None, "out"),
        P(None, "inp", "out"),
        P(),
        P("out"),
        P(),
        P(None, "inp", "out"),
        P(),
        P("out"),
    )
    return jax.shard_map(
        per_device,
        mesh=mesh,
        in_specs=placed,
        out_specs=(P(None, "out"), P("inp", "out")),
        check_vma=False,
    )
```
